16 devices in a mesh: dp: 2 (over y, z), tp: 8 (over x, core).
Axes of the slice: x: 4, y: 2, z: 1, core: 2. Of those that a mesh axis runs over, the one named last changes fastest.
The devices are a block of a 4x4x8 slice.
Arguments:
- hidden: bfloat16 [2048, 2048], P('dp'), parts along dimension 0
- w_q: bfloat16 [2048, 2048], P(None, 'tp')
- w_k: bfloat16 [2048, 2048], P(None, 'tp')
- w_v: bfloat16 [2048, 2048], P(None, 'tp')
- w_o: bfloat16 [2048, 2048], P('tp')
- q_norm_w: float32 [2048], P('tp')
- k_norm_w: float32 [2048], P('tp')
- post_norm_w: float32 [2048], replicated
- k_cache: bfloat16 [2048, 32, 16, 128], P('dp', None, 'tp'), parts along dimension 0
- v_cache: bfloat16 [2048, 32, 16, 128], P('dp', None, 'tp'), parts along dimension 0
- positions: int32 [2048], P('dp'), parts along dimension 0
Outputs:
- output 1: bfloat16 [2048, 2048], P('dp'), parts along dimension 0
- output 2: bfloat16 [2048, 32, 16, 128], P('dp', None, 'tp'), parts along dimension 0
- output 3: bfloat16 [2048, 32, 16, 128], P('dp', None, 'tp'), parts along dimension 0
There are 2 independent parts. The reference program is written for one: setup_inputs(seed, part) draws one part's arguments, and reference() takes and returns one part's arrays. A program takes and returns all parts, laid end to end along the dimension named above; an argument that names none is the same for every part.
All inputs are finite; a program needn't handle non-finite values.
Results may differ from the reference program's by a relative error of at most 0.0111559.
Values are sent between devices in bfloat16 or wider.
A program may use at most 768 MiB of HBM per device.

```python
import jax
import jax.numpy as jnp
from jax import lax

BATCH = 1024
CACHE_LEN = 32
HEADS = 16
HEAD_DIM = 128
WIDTH = HEADS * HEAD_DIM
NORM_EPS = 1e-6
ROPE_BASE = 500000.0


def setup_inputs(seed: int = 0, part: int = 0) -> dict:
    base_key = jax.random.key(seed)
    shared_keys = jax.random.split(base_key, 9)
    part_keys = jax.random.split(jax.random.fold_in(base_key, part), 6)
    fan_scale = WIDTH ** -0.5
    head_frac = jnp.arange(HEADS, dtype=jnp.float32) / max(HEADS - 1, 1)
    q_heads = jnp.exp(1.2 * (2.0 * head_frac - 1.0) + 0.2 * jax.random.normal(shared_keys[0], (HEADS,)))
    k_heads = jnp.exp(1.2 * (1.0 - 2.0 * head_frac) + 0.2 * jax.random.normal(shared_keys[1], (HEADS,)))
    q_cols = jnp.repeat(q_heads, HEAD_DIM)
    k_cols = jnp.repeat(k_heads, HEAD_DIM)
    w_q = (jax.random.normal(shared_keys[2], (WIDTH, WIDTH)) * fan_scale * q_cols[None, :]).astype(jnp.bfloat16)
    w_k = (jax.random.normal(shared_keys[3], (WIDTH, WIDTH)) * fan_scale * k_cols[None, :]).astype(jnp.bfloat16)
    w_v = (jax.random.normal(shared_keys[4], (WIDTH, WIDTH)) * fan_scale).astype(jnp.bfloat16)
    w_o = (jax.random.normal(shared_keys[5], (WIDTH, WIDTH)) * fan_scale).astype(jnp.bfloat16)
    q_norm_w = jax.random.uniform(shared_keys[6], (WIDTH,), minval=0.5, maxval=1.5).astype(jnp.float32)
    k_norm_w = jax.random.uniform(shared_keys[7], (WIDTH,), minval=0.5, maxval=1.5).astype(jnp.float32)
    post_norm_w = jax.random.uniform(shared_keys[8], (WIDTH,), minval=0.5, maxval=1.5).astype(jnp.float32)
    hidden = jax.random.normal(part_keys[0], (BATCH, WIDTH)).astype(jnp.bfloat16)
    k_cache = jax.random.normal(part_keys[1], (BATCH, CACHE_LEN, HEADS, HEAD_DIM)).astype(jnp.bfloat16)
    v_cache = jax.random.normal(part_keys[2], (BATCH, CACHE_LEN, HEADS, HEAD_DIM)).astype(jnp.bfloat16)
    slot_draw = jax.random.randint(part_keys[3], (BATCH,), 0, CACHE_LEN, dtype=jnp.int32)
    shift_bits = jax.random.randint(part_keys[4], (BATCH,), 0, 10, dtype=jnp.int32)
    longest = jax.random.randint(part_keys[5], (), 0, BATCH, dtype=jnp.int32)
    positions = jnp.where(jnp.arange(BATCH, dtype=jnp.int32) == longest, CACHE_LEN - 1, jnp.right_shift(slot_draw, shift_bits)).astype(jnp.int32)
    return dict(hidden=hidden, w_q=w_q, w_k=w_k, w_v=w_v, w_o=w_o, q_norm_w=q_norm_w, k_norm_w=k_norm_w, post_norm_w=post_norm_w, k_cache=k_cache, v_cache=v_cache, positions=positions)


def width_norm(vals, gain):
    wide = vals.astype(jnp.float32)
    inv_rms = lax.rsqrt(jnp.mean(wide * wide, axis=-1, keepdims=True) + NORM_EPS)
    return wide * inv_rms * gain


def apply_rope(heads_val, positions):
    half = HEAD_DIM // 2
    inv_freq = ROPE_BASE ** (-2.0 * jnp.arange(half, dtype=jnp.float32) / HEAD_DIM)
    angles = positions.astype(jnp.float32)[:, None, None] * inv_freq[None, None, :]
    cos_tab = jnp.cos(angles)
    sin_tab = jnp.sin(angles)
    wide = heads_val.astype(jnp.float32)
    first = wide[..., :half]
    second = wide[..., half:]
    return jnp.concatenate([first * cos_tab - second * sin_tab, second * cos_tab + first * sin_tab], axis=-1).astype(jnp.bfloat16)


def attend_row(row_args):
    q_row, k_row, v_row, row_pos = row_args
    slot_ids = jnp.arange(CACHE_LEN)
    scores = jnp.einsum('hd,shd->hs', q_row.astype(jnp.float32), k_row.astype(jnp.float32)) * HEAD_DIM ** -0.5
    scores = jnp.where(slot_ids[None, :] <= row_pos, scores, -1e30)
    probs = jax.nn.softmax(scores, axis=-1).astype(jnp.bfloat16)
    return jnp.einsum('hs,shd->hd', probs.astype(jnp.float32), v_row.astype(jnp.float32)).astype(jnp.bfloat16)


def reference(hidden, w_q, w_k, w_v, w_o, q_norm_w, k_norm_w, post_norm_w, k_cache, v_cache, positions):
    n_rows = hidden.shape[0]
    q_full = jnp.dot(hidden, w_q, preferred_element_type=jnp.float32).astype(jnp.bfloat16)
    k_full = jnp.dot(hidden, w_k, preferred_element_type=jnp.float32).astype(jnp.bfloat16)
    v_full = jnp.dot(hidden, w_v, preferred_element_type=jnp.float32).astype(jnp.bfloat16)
    q_normed = width_norm(q_full, q_norm_w).astype(jnp.bfloat16).reshape(n_rows, HEADS, HEAD_DIM)
    k_normed = width_norm(k_full, k_norm_w).astype(jnp.bfloat16).reshape(n_rows, HEADS, HEAD_DIM)
    q_rot = apply_rope(q_normed, positions)
    k_rot = apply_rope(k_normed, positions)
    v_heads = v_full.reshape(n_rows, HEADS, HEAD_DIM)
    at_slot = (jnp.arange(CACHE_LEN)[None, :] == positions[:, None])[:, :, None, None]
    k_new = jnp.where(at_slot, k_rot[:, None], k_cache)
    v_new = jnp.where(at_slot, v_heads[:, None], v_cache)
    attn = lax.map(attend_row, (q_rot, k_new, v_new, positions))
    a_out = jnp.dot(attn.reshape(n_rows, WIDTH), w_o, preferred_element_type=jnp.float32)
    hidden_out = (hidden.astype(jnp.float32) + width_norm(a_out, post_norm_w)).astype(jnp.bfloat16)
    return hidden_out, k_new, v_new
```

```python
import functools
import math

import jax
import jax.numpy as jnp
import numpy as np
from jax import lax
from jax.experimental import pallas as pl
from jax.experimental.pallas import tpu as pltpu
from jax.sharding import PartitionSpec as P

NEG = -1e30

def attn_kernel(blk, nbuf, ahead, pos_s, pos_v, q_ref, kn_ref, vn_ref, kc_hbm, vc_hbm,
                o_ref, ko_hbm, vo_hbm, kbuf, vbuf, pcol, isem, osem):
    rows = q_ref.shape[0] * 8
    slots, heads, hd = kc_hbm.shape[1:]
    n_blk = rows // blk
    per_row = slots * heads
    scale2 = (hd ** -0.5) * math.log2(math.e)

    def cin(i, s):
        sl = pl.ds(i * blk, blk)
        return (pltpu.make_async_copy(kc_hbm.at[sl], kbuf.at[s], isem.at[0, s]),
                pltpu.make_async_copy(vc_hbm.at[sl], vbuf.at[s], isem.at[1, s]))

    def cout(i, s):
        sl = pl.ds(i * blk, blk)
        return (pltpu.make_async_copy(kbuf.at[s], ko_hbm.at[sl], osem.at[0, s]),
                pltpu.make_async_copy(vbuf.at[s], vo_hbm.at[sl], osem.at[1, s]))

    for j in range(ahead):
        for c in cin(j, j):
            c.start()

    lane = lax.broadcasted_iota(jnp.int32, (128, 128), 1)
    sub = lax.broadcasted_iota(jnp.int32, (128, 128), 0)
    for b in range(rows // 128):
        row = jnp.broadcast_to(pos_v[b:b + 1, :], (128, 128))
        col = jnp.sum(jnp.where(lane == sub, row, 0).astype(jnp.float32), axis=1, keepdims=True)
        pcol[pl.ds(b * 128, 128), :] = jnp.broadcast_to(col.astype(jnp.int32), (128, 128))

    ci = lax.broadcasted_iota(jnp.int32, (16, 8 * per_row), 1)
    ri = lax.broadcasted_iota(jnp.int32, (16, 8 * per_row), 0)
    match = jnp.logical_and(ci // per_row == ri % 8, ci % 2 == ri // 8)
    slotm = jnp.where(match, (ci % per_row) // 2, 1000)

    def body(i, carry):
        s = lax.rem(i, nbuf)
        nxt = i + ahead

        @pl.when(nxt < n_blk)
        def _():
            sn = lax.rem(nxt, nbuf)

            @pl.when(nxt >= nbuf)
            def _():
                for c in cout(0, sn):
                    c.wait()
            for c in cin(nxt, sn):
                c.start()
        for c in cin(0, s):
            c.wait()
        base = i * blk
        for r in range(blk):
            p = pos_s[base + r]
            kbuf[s, r, p] = kn_ref[base + r]
            vbuf[s, r, p] = vn_ref[base + r]
        kf = kbuf.at[s].reshape(blk * per_row, hd)
        vf = vbuf.at[s].reshape(blk * per_row, hd)
        for pair in range(blk // 16):
            ps = []
            for g in (2 * pair, 2 * pair + 1):
                qg = q_ref[i * (blk // 8) + g]
                kg = kf[pl.ds(g * 8 * per_row, 8 * per_row), :]
                sc = lax.dot_general(qg, kg, (((1,), (1,)), ((), ())), preferred_element_type=jnp.float32)
                pc = pcol[pl.ds(pl.multiple_of(base + g * 8, 8), 8), :]
                pc = jnp.concatenate([pc, pc], axis=0)
                pc = jnp.concatenate([pc] * (8 * per_row // 128), axis=1)
                sc = jnp.where(slotm <= pc, sc, NEG)
                m = jnp.max(sc, axis=1, keepdims=True)
                e = jnp.exp2((sc - m) * scale2)
                l = jnp.sum(e, axis=1, keepdims=True)
                ps.append((e / l).astype(jnp.bfloat16))
            pp = jnp.concatenate(ps, axis=0)
            va = vf[pl.ds(2 * pair * 8 * per_row, 8 * per_row), :]
            vb = vf[pl.ds((2 * pair + 1) * 8 * per_row, 8 * per_row), :]
            vv = jnp.concatenate([va, vb], axis=1)
            oo = jnp.dot(pp, vv, preferred_element_type=jnp.float32)
            h0 = jnp.concatenate([oo[0:8, :hd], oo[16:24, hd:]], axis=0)
            h1 = jnp.concatenate([oo[8:16, :hd], oo[24:32, hd:]], axis=0)
            rs = pl.ds(pl.multiple_of(base + pair * 16, 16), 16)
            o_ref[rs, 0:hd] = h0.astype(jnp.bfloat16)
            o_ref[rs, hd:2 * hd] = h1.astype(jnp.bfloat16)
        for c in cout(i, s):
            c.start()
        return carry

    lax.fori_loop(0, n_blk, body, 0)
    for j in range(min(nbuf, n_blk)):
        for c in cout(0, (n_blk - 1 - j) % nbuf):
            c.wait()


def attention(positions, qg, kn, vn, k_cache, v_cache, blk=64, nbuf=4, ahead=2):
    rows, slots, heads, hd = k_cache.shape
    vm = pl.BlockSpec(memory_space=pltpu.VMEM)
    anyspec = pl.BlockSpec(memory_space=pl.ANY)
    return pl.pallas_call(
        functools.partial(attn_kernel, blk, nbuf, ahead),
        out_shape=(jax.ShapeDtypeStruct((rows, heads * hd), jnp.bfloat16),
                   jax.ShapeDtypeStruct(k_cache.shape, k_cache.dtype),
                   jax.ShapeDtypeStruct(v_cache.shape, v_cache.dtype)),
        in_specs=[pl.BlockSpec(memory_space=pltpu.SMEM), vm, vm, vm, vm, anyspec, anyspec],
        out_specs=(vm, anyspec, anyspec),
        scratch_shapes=[
            pltpu.VMEM((nbuf, blk, slots, heads, hd), jnp.bfloat16),
            pltpu.VMEM((nbuf, blk, slots, heads, hd), jnp.bfloat16),
            pltpu.VMEM((rows, 128), jnp.int32),
            pltpu.SemaphoreType.DMA((2, nbuf)),
            pltpu.SemaphoreType.DMA((2, nbuf)),
        ],
        name='attn',
    )(positions, positions.reshape(rows // 128, 128), qg, kn, vn, k_cache, v_cache)


NORM_EPS = 1e-6
ROPE_BASE = 500000.0
MESH = pl.DeviceIdType.MESH
VMEM_SPEC = pl.BlockSpec(memory_space=pltpu.VMEM)
ANY_SPEC = pl.BlockSpec(memory_space=pl.ANY)
LANES = 128


def rope_table(slots, head_dim):
    half = head_dim // 2
    inv_freq = np.float32(ROPE_BASE) ** (np.float32(-2.0) * np.arange(half, dtype=np.float32) / np.float32(head_dim))
    angles = (np.arange(slots, dtype=np.float32)[:, None] * inv_freq[None, :].astype(np.float32)).astype(np.float64)
    cos, sin = np.cos(angles).astype(np.float32), np.sin(angles).astype(np.float32)
    full = np.concatenate([cos, cos, -sin, sin], axis=1)
    parts, rest = [], full
    for _ in range(3):
        part = rest.astype(jnp.bfloat16)
        parts.append(part)
        rest = rest - part.astype(np.float32)
    pad = np.zeros((LANES - 3 * slots, full.shape[1]), jnp.bfloat16)
    return np.concatenate(parts + [pad], axis=0)


def qkv_kernel(n, chunk, slots, pos_ref, tab_ref, qw_ref, kw_ref, hid_hbm, wq_hbm, wk_hbm, wv_hbm, wo_hbm,
               qg_ref, kn_ref, vn_ref, wop_hbm,
               hid, wq, wk, wv, qf, kf, stage, esend, erecv, lsem, osem, ssem, rsem):
    me = lax.axis_index('tp')
    rows, width = hid_hbm.shape
    cols = wq_hbm.shape[1]
    hd = qg_ref.shape[2]
    n_chunk = rows // chunk
    per = chunk // LANES

    loads = [pltpu.make_async_copy(wq_hbm, wq, lsem.at[0])]
    loads.append(pltpu.make_async_copy(hid_hbm.at[pl.ds(0, chunk)], hid.at[pl.ds(0, chunk)], lsem.at[3]))
    loads.append(pltpu.make_async_copy(wk_hbm, wk, lsem.at[1]))
    for c in range(1, n_chunk):
        loads.append(pltpu.make_async_copy(hid_hbm.at[pl.ds(c * chunk, chunk)], hid.at[pl.ds(c * chunk, chunk)], lsem.at[3 + c]))
    loads.append(pltpu.make_async_copy(wv_hbm, wv, lsem.at[2]))
    for cp in loads:
        cp.start()

    barrier = pltpu.get_barrier_semaphore()
    for d in range(1, n):
        pl.semaphore_signal(barrier, inc=1, device_id={'tp': lax.rem(me + d, n)}, device_id_type=MESH)

    lane = lax.broadcasted_iota(jnp.int32, (LANES, LANES), 1)
    sub = lax.broadcasted_iota(jnp.int32, (LANES, LANES), 0)
    eye = lane == sub

    def to_row(col):
        return jnp.sum(jnp.where(eye, jnp.broadcast_to(col, (LANES, LANES)), 0.0), axis=0, keepdims=True)

    def to_col(row):
        return jnp.sum(jnp.where(eye, jnp.broadcast_to(row, (LANES, LANES)), 0.0), axis=1, keepdims=True)

    def energy_copy(c, d):
        return pltpu.make_async_remote_copy(
            src_ref=esend.at[c], dst_ref=erecv.at[c, d - 1], send_sem=ssem.at[c, d - 1], recv_sem=rsem.at[c, d - 1],
            device_id={'tp': lax.rem(me + d, n)}, device_id_type=MESH)

    wo_copy = pltpu.make_async_remote_copy(
        src_ref=wo_hbm, dst_ref=wop_hbm, send_sem=osem.at[0], recv_sem=osem.at[1],
        device_id={'tp': me + 1 - 2 * lax.rem(me, 2)}, device_id_type=MESH)

    loads[0].wait()
    for c in range(n_chunk):
        loads[1 if c == 0 else 2 + c].wait()
        cs = pl.ds(c * chunk, chunk)
        rows_out = []
        for w, f, first in ((wq, qf, 0), (wk, kf, 1)):
            if c == 0 and first == 1:
                loads[2].wait()
            val = jnp.dot(hid[cs, :], w[...], preferred_element_type=jnp.float32).astype(jnp.bfloat16).astype(jnp.float32)
            f[cs, :] = val
            en = jnp.sum(val * val, axis=1, keepdims=True)
            for b in range(per):
                rows_out.append(to_row(en[b * LANES:(b + 1) * LANES]))
        pad = 8 - len(rows_out)
        esend[c] = jnp.concatenate(rows_out + [jnp.zeros((pad, LANES), jnp.float32)], axis=0)
        if c == 0:
            pl.semaphore_wait(barrier, n - 1)
            wo_copy.start()
        for d in range(1, n):
            energy_copy(c, d).start()

    loads[-1].wait()
    for c in range(n_chunk):
        cs = pl.ds(c * chunk, chunk)
        val = jnp.dot(hid[cs, :], wv[...], preferred_element_type=jnp.float32)
        stage[pl.ds(0, chunk, stride=2), :] = val[:, :hd]
        stage[pl.ds(1, chunk, stride=2), :] = val[:, hd:]
        vn_ref[pl.ds(c * 2 * chunk, 2 * chunk), :] = stage[...].astype(jnp.bfloat16)

    for c in range(n_chunk):
        total = esend[c]
        for d in range(1, n):
            energy_copy(c, d).wait_recv()
            total = total + erecv[c, d - 1]
        inv = lax.rsqrt(total / width + NORM_EPS)
        for b in range(per):
            base = c * chunk + b * LANES
            rs = pl.ds(base, LANES)
            p = to_col(pos_ref[c * per + b:c * per + b + 1, :].astype(jnp.float32)).astype(jnp.int32)
            hot = jnp.logical_and(lane < 3 * slots, lane % slots == p)
            trig = jnp.dot(jnp.where(hot, 1.0, 0.0).astype(jnp.bfloat16), tab_ref[...], preferred_element_type=jnp.float32)
            cos, sin = trig[:, :hd], trig[:, hd:]
            for f, w_ref, which in ((qf, qw_ref, 0), (kf, kw_ref, 1)):
                scale = to_col(inv[which * per + b:which * per + b + 1, :])
                normed = (f[rs, :] * scale * w_ref[...]).astype(jnp.bfloat16).astype(jnp.float32)
                rot = []
                for h in range(cols // hd):
                    x = normed[:, h * hd:(h + 1) * hd]
                    rot.append(x * cos + pltpu.roll(x, hd // 2, 1) * sin)
                if which == 0:
                    grouped = jnp.concatenate([r.reshape(LANES // 8, 8, hd) for r in rot], axis=1)
                    qg_ref[pl.ds(base // 8, LANES // 8)] = grouped.astype(jnp.bfloat16)
                else:
                    stage[pl.ds(0, LANES, stride=2), :] = rot[0]
                    stage[pl.ds(1, LANES, stride=2), :] = rot[1]
                    kn_ref[pl.ds(2 * base, 2 * LANES), :] = stage[pl.ds(0, 2 * LANES), :].astype(jnp.bfloat16)

    for c in range(n_chunk):
        for d in range(1, n):
            energy_copy(c, d).wait_send()
    wo_copy.wait()


def qkv(n, slots, heads, hd, positions, hidden, w_q, w_k, w_v, w_o, q_norm_w, k_norm_w, chunk=256):
    rows, width = hidden.shape
    cols = heads * hd
    n_chunk = rows // chunk
    f32, bf16 = jnp.float32, jnp.bfloat16
    return pl.pallas_call(
        functools.partial(qkv_kernel, n, chunk, slots),
        out_shape=(jax.ShapeDtypeStruct((rows // 8, 16, hd), bf16), jax.ShapeDtypeStruct((2 * rows, hd), bf16),
                   jax.ShapeDtypeStruct((2 * rows, hd), bf16), jax.ShapeDtypeStruct(w_o.shape, bf16)),
        in_specs=[VMEM_SPEC] * 4 + [ANY_SPEC] * 5,
        out_specs=(VMEM_SPEC, VMEM_SPEC, VMEM_SPEC, ANY_SPEC),
        scratch_shapes=[
            pltpu.VMEM((rows, width), bf16), pltpu.VMEM((width, cols), bf16), pltpu.VMEM((width, cols), bf16),
            pltpu.VMEM((width, cols), bf16), pltpu.VMEM((rows, cols), f32), pltpu.VMEM((rows, cols), f32),
            pltpu.VMEM((2 * chunk, hd), f32), pltpu.VMEM((n_chunk, 8, LANES), f32),
            pltpu.VMEM((n_chunk, n - 1, 8, LANES), f32),
            pltpu.SemaphoreType.DMA((3 + n_chunk,)), pltpu.SemaphoreType.DMA((2,)),
            pltpu.SemaphoreType.DMA((n_chunk, n - 1)), pltpu.SemaphoreType.DMA((n_chunk, n - 1)),
        ],
        compiler_params=pltpu.CompilerParams(collective_id=0, has_side_effects=True),
        name='qkv',
    )(positions.reshape(rows // LANES, LANES), jnp.asarray(rope_table(slots, hd)), q_norm_w.reshape(1, cols),
      k_norm_w.reshape(1, cols), hidden, w_q, w_k, w_v, w_o)


O, A_R, A_L, B_R, B_L, C_R, C_L, G1_R, G1_L, G2_R, G2_L, D_OWN, D_LEFT, D_RIGHT, D_ANT0, D_ANT1 = range(16)


def out_kernel(n, nj, o_ref, pw_ref, hid_hbm, wo_hbm, wop_hbm, out_ref,
               wo, wop, opart, part, hid, ra, rb, rc, cst, lsem, ssem, rsem):
    me = lax.axis_index('tp')
    nchip = n // 2
    chip, core = me // 2, lax.rem(me, 2)
    rows, width = out_ref.shape
    rc_rows = rows // nj
    half_rows = rc_rows // 2
    own = half_rows // nchip
    hf = own // 2
    xr, xl, xa = lax.rem(chip + 1, nchip), lax.rem(chip + nchip - 1, nchip), lax.rem(chip + 2, nchip)
    right, left, mate = xr * 2 + core, xl * 2 + core, chip * 2 + (1 - core)

    def qs(y, part_no, count):
        return pl.ds(pl.multiple_of(y * own + part_no * hf, hf), count)

    def gs(j, c, y, part_no, count):
        return pl.ds(pl.multiple_of(j * rc_rows + c * half_rows + y * own + part_no * hf, hf), count)

    def remote(kind, j, src, dst, dev):
        return pltpu.make_async_remote_copy(src_ref=src, dst_ref=dst, send_sem=ssem.at[kind, j], recv_sem=rsem.at[kind, j],
                                            device_id={'tp': dev}, device_id_type=MESH)

    sent = []

    def send(kind, j, src, dst, dev):
        cp = remote(kind, j, src, dst, dev)
        cp.start()
        sent.append(cp)

    def recv(kind, j, dst, dev):
        remote(kind, j, dst, dst, dev).wait_recv()

    lw = [pltpu.make_async_copy(wo_hbm, wo, lsem.at[0]), pltpu.make_async_copy(wop_hbm, wop, lsem.at[1])]
    lh = [pltpu.make_async_copy(hid_hbm.at[gs(j, core, chip, 0, own)], hid.at[j], lsem.at[2 + j]) for j in range(nj)]
    for cp in lw + lh:
        cp.start()

    barrier = pltpu.get_barrier_semaphore()
    for dev in (right, left, mate):
        pl.semaphore_signal(barrier, inc=1, device_id={'tp': dev}, device_id_type=MESH)
    pl.semaphore_wait(barrier, 3)

    for j in range(nj):
        src = pl.ds(pl.multiple_of(j * rc_rows + (1 - core) * half_rows, half_rows), half_rows)
        send(O, j, o_ref.at[src], opart.at[j], mate)

    def p1(j):
        if j == 0:
            lw[0].wait()
            lw[1].wait()
        recv(O, j, opart.at[j], mate)
        mine = o_ref[pl.ds(pl.multiple_of(j * rc_rows + core * half_rows, half_rows), half_rows), :]
        theirs = opart[j]
        step = 512
        for c0 in range(0, width, step):
            acc = jnp.dot(mine, wo[:, c0:c0 + step], preferred_element_type=jnp.float32)
            acc = acc + jnp.dot(theirs, wop[:, c0:c0 + step], preferred_element_type=jnp.float32)
            part[j, :, c0:c0 + step] = acc.astype(jnp.bfloat16)
        send(A_R, j, part.at[j, qs(xa, 0, hf)], ra.at[j, 0], right)
        send(A_L, j, part.at[j, qs(xa, 1, hf)], ra.at[j, 1], left)
        send(B_R, j, part.at[j, qs(xr, 1, hf)], rb.at[j, 0], right)
        send(B_L, j, part.at[j, qs(xl, 0, hf)], rb.at[j, 1], left)

    def p2(j):
        recv(A_R, j, ra.at[j, 0], left)
        cst[j, 0] = (part[j, qs(xr, 0, hf), :].astype(jnp.float32) + ra[j, 0].astype(jnp.float32)).astype(jnp.bfloat16)
        send(C_R, j, cst.at[j, 0], rc.at[j, 0], right)
        recv(A_L, j, ra.at[j, 1], right)
        cst[j, 1] = (part[j, qs(xl, 1, hf), :].astype(jnp.float32) + ra[j, 1].astype(jnp.float32)).astype(jnp.bfloat16)
        send(C_L, j, cst.at[j, 1], rc.at[j, 1], left)

    def p3(j):
        lh[j].wait()
        for k in range(2):
            recv((C_R, C_L)[k], j, rc.at[j, k], (left, right)[k])
            recv((B_L, B_R)[k], j, rb.at[j, 1 - k], (right, left)[k])
            a = (part[j, qs(chip, k, hf), :].astype(jnp.float32) + rc[j, k].astype(jnp.float32)
                 + rb[j, 1 - k].astype(jnp.float32))
            inv = lax.rsqrt(jnp.sum(a * a, axis=1, keepdims=True) / width + NORM_EPS)
            x = hid[j, k * hf:(k + 1) * hf, :].astype(jnp.float32)
            out_ref[gs(j, core, chip, k, hf), :] = (x + a * inv * pw_ref[...]).astype(jnp.bfloat16)
        blk = out_ref.at[gs(j, core, chip, 0, own)]
        send(G1_R, j, blk, blk, right)
        send(G1_L, j, blk, blk, left)
        send(D_OWN, j, blk, blk, mate)

    def p4(j):
        bl = out_ref.at[gs(j, core, xl, 0, own)]
        br = out_ref.at[gs(j, core, xr, 0, own)]
        recv(G1_R, j, bl, left)
        fl = out_ref.at[gs(j, core, xl, 0, hf)]
        send(G2_R, j, fl, fl, right)
        send(D_LEFT, j, bl, bl, mate)
        recv(G1_L, j, br, right)
        fr = out_ref.at[gs(j, core, xr, 1, hf)]
        send(G2_L, j, fr, fr, left)
        send(D_RIGHT, j, br, br, mate)

    def p5(j):
        b0 = out_ref.at[gs(j, core, xa, 0, hf)]
        recv(G2_R, j, b0, left)
        send(D_ANT0, j, b0, b0, mate)
        b1 = out_ref.at[gs(j, core, xa, 1, hf)]
        recv(G2_L, j, b1, right)
        send(D_ANT1, j, b1, b1, mate)

    stages = (p1, p2, p3, p4, p5)
    for t in range(nj + len(stages) - 1):
        for s, fn in enumerate(stages):
            if 0 <= t - s < nj:
                fn(t - s)
    for j in range(nj):
        oc = 1 - core
        recv(D_OWN, j, out_ref.at[gs(j, oc, chip, 0, own)], mate)
        recv(D_LEFT, j, out_ref.at[gs(j, oc, xl, 0, own)], mate)
        recv(D_RIGHT, j, out_ref.at[gs(j, oc, xr, 0, own)], mate)
        recv(D_ANT0, j, out_ref.at[gs(j, oc, xa, 0, hf)], mate)
        recv(D_ANT1, j, out_ref.at[gs(j, oc, xa, 1, hf)], mate)
    for cp in sent:
        cp.wait_send()


def project(n, attn, post_norm_w, hidden, w_o, w_o_mate, nj=4):
    rows, width = hidden.shape
    cols = attn.shape[1]
    half = rows // nj // 2
    own = half // (n // 2)
    hf = own // 2
    bf16 = jnp.bfloat16
    return pl.pallas_call(
        functools.partial(out_kernel, n, nj),
        out_shape=jax.ShapeDtypeStruct((rows, width), bf16),
        in_specs=[VMEM_SPEC, VMEM_SPEC, ANY_SPEC, ANY_SPEC, ANY_SPEC],
        out_specs=VMEM_SPEC,
        scratch_shapes=[
            pltpu.VMEM((cols, width), bf16), pltpu.VMEM((cols, width), bf16), pltpu.VMEM((nj, half, cols), bf16),
            pltpu.VMEM((nj, half, width), bf16), pltpu.VMEM((nj, own, width), bf16),
            pltpu.VMEM((nj, 2, hf, width), bf16), pltpu.VMEM((nj, 2, hf, width), bf16),
            pltpu.VMEM((nj, 2, hf, width), bf16), pltpu.VMEM((nj, 2, hf, width), bf16),
            pltpu.SemaphoreType.DMA((2 + nj,)), pltpu.SemaphoreType.DMA((16, nj)), pltpu.SemaphoreType.DMA((16, nj)),
        ],
        compiler_params=pltpu.CompilerParams(collective_id=1, has_side_effects=True),
        name='project',
    )(attn, post_norm_w.reshape(1, width), hidden, w_o, w_o_mate)


def solution(mesh):
    n = mesh.shape['tp']

    def local_step(hidden, w_q, w_k, w_v, w_o, q_norm_w, k_norm_w, post_norm_w, k_cache, v_cache, positions):
        rows, slots, heads, hd = k_cache.shape
        qg, kn, vn, w_o_mate = qkv(n, slots, heads, hd, positions, hidden, w_q, w_k, w_v, w_o, q_norm_w, k_norm_w)
        attn, k_new, v_new = attention(positions, qg, kn.reshape(rows, heads, hd), vn.reshape(rows, heads, hd), k_cache, v_cache)
        hidden_out = project(n, attn, post_norm_w, hidden, w_o, w_o_mate)
        return hidden_out, k_new, v_new

    cache_spec = P('dp', None, 'tp', None)
    return jax.shard_map(local_step, mesh=mesh, in_specs=(P('dp', None), P(None, 'tp'), P(None, 'tp'), P(None, 'tp'), P('tp', None), P('tp'), P('tp'), P(None), cache_spec, cache_spec, P('dp')), out_specs=(P('dp', None), cache_spec, cache_spec), check_vma=False)
```

```python
import functools
import math

import jax
import jax.numpy as jnp
import numpy as np
from jax import lax
from jax.experimental import pallas as pl
from jax.experimental.pallas import tpu as pltpu
from jax.sharding import PartitionSpec as P

NORM_EPS = 1e-6
ROPE_BASE = 500000.0
NEG = -1e30
MESH = pl.DeviceIdType.MESH
VMEM_SPEC = pl.BlockSpec(memory_space=pltpu.VMEM)
HBM_SPEC = pl.BlockSpec(memory_space=pltpu.HBM)
LANES = 128
BLK = 64


def rope_table(slots, head_dim):
    half = head_dim // 2
    inv_freq = np.float32(ROPE_BASE) ** (np.float32(-2.0) * np.arange(half, dtype=np.float32) / np.float32(head_dim))
    angles = (np.arange(slots, dtype=np.float32)[:, None] * inv_freq[None, :].astype(np.float32)).astype(np.float64)
    cos, sin = np.cos(angles).astype(np.float32), np.sin(angles).astype(np.float32)
    full = np.concatenate([cos, cos, -sin, sin], axis=1)
    parts, rest = [], full
    for _ in range(3):
        part = rest.astype(jnp.bfloat16)
        parts.append(part)
        rest = rest - part.astype(np.float32)
    pad = np.zeros((LANES - 3 * slots, full.shape[1]), jnp.bfloat16)
    return np.concatenate(parts + [pad], axis=0)


O, A_R, A_L, B_R, B_L, C_R, C_L, G1_R, G1_L, G2_R, G2_L, D_OWN, D_LEFT, D_RIGHT, D_ANT0, D_ANT1 = range(16)


def step_kernel(n, nj, slots, heads, hd,
                pos_ref, tab_ref, qw_ref, kw_ref, pw_ref, hid_hbm, wq_hbm, wk_hbm, wv_hbm, wo_hbm, kc_hbm, vc_hbm,
                kc, vc, out_ref, kn_hbm, vn_hbm,
                kn, vn, hid, wq, wk, wv, wo, wop, qf, kf, qg, pcol, s_scr, p_scr, o_scr, opart, part, ra, rb, rc, cst,
                esend, erecv, lsem, csem, nsem, osem, essem, ersem, ssem, rsem):
    me = lax.axis_index('tp')
    rows, width = hid_hbm.shape
    cols = heads * hd
    per_row = slots * heads
    rc_rows = rows // nj
    per = rc_rows // LANES
    nchip = n // 2
    chip, core = me // 2, lax.rem(me, 2)
    half_rows = rc_rows // 2
    own = half_rows // nchip
    hf = own // 2
    xr, xl, xa = lax.rem(chip + 1, nchip), lax.rem(chip + nchip - 1, nchip), lax.rem(chip + 2, nchip)
    right, left, mate = xr * 2 + core, xl * 2 + core, chip * 2 + (1 - core)
    f32, bf16 = jnp.float32, jnp.bfloat16

    def chunk(c):
        return pl.ds(c * rc_rows, rc_rows)

    ld_w = [pltpu.make_async_copy(src, dst, lsem.at[k]) for k, (src, dst) in
            enumerate(((wq_hbm, wq), (wk_hbm, wk), (wv_hbm, wv), (wo_hbm, wo)))]
    ld_h = [pltpu.make_async_copy(hid_hbm.at[chunk(c)], hid.at[chunk(c)], lsem.at[4 + c]) for c in range(nj)]

    def ld_kv(c):
        sl = pl.ds(c * rc_rows * per_row, rc_rows * per_row)
        return [pltpu.make_async_copy(kc_hbm.at[sl], kc.at[sl], csem.at[0, c]),
                pltpu.make_async_copy(vc_hbm.at[sl], vc.at[sl], csem.at[1, c])]

    for cp in (ld_h[0], ld_w[0], ld_w[1], ld_w[2], ld_h[1]):
        cp.start()

    barrier = pltpu.get_barrier_semaphore()
    for d in range(1, n):
        pl.semaphore_signal(barrier, inc=1, device_id={'tp': lax.rem(me + d, n)}, device_id_type=MESH)

    lane = lax.broadcasted_iota(jnp.int32, (LANES, LANES), 1)
    sub = lax.broadcasted_iota(jnp.int32, (LANES, LANES), 0)
    eye = lane == sub
    span = 8 * per_row
    ci = lax.broadcasted_iota(jnp.int32, (16, span), 1)
    ri = lax.broadcasted_iota(jnp.int32, (16, span), 0)
    match = jnp.logical_and(ci // per_row == ri % 8, ci % heads == ri // 8)
    slotm = jnp.where(match, (ci % per_row) // heads, 1000)
    scale2 = (hd ** -0.5) * math.log2(math.e)

    def to_row(col):
        return jnp.sum(jnp.where(eye, jnp.broadcast_to(col, (LANES, LANES)), 0.0), axis=0, keepdims=True)

    def to_col(row):
        return jnp.sum(jnp.where(eye, jnp.broadcast_to(row, (LANES, LANES)), 0.0), axis=1, keepdims=True)

    def energy_copy(c, d):
        return pltpu.make_async_remote_copy(
            src_ref=esend.at[c], dst_ref=erecv.at[c, d - 1], send_sem=essem.at[c, d - 1], recv_sem=ersem.at[c, d - 1],
            device_id={'tp': lax.rem(me + d, n)}, device_id_type=MESH)

    wo_copy = pltpu.make_async_remote_copy(
        src_ref=wo_hbm, dst_ref=wop, send_sem=osem.at[0], recv_sem=osem.at[1],
        device_id={'tp': mate}, device_id_type=MESH)

    def project_qkv(c):
        cs = chunk(c)
        ld_h[c].wait()
        rows_out = []
        for k, (w, f) in enumerate(((wq, qf), (wk, kf))):
            if c == 0:
                ld_w[k].wait()
            val = jnp.dot(hid[cs, :], w[...], preferred_element_type=f32).astype(bf16).astype(f32)
            f[cs, :] = val
            en = jnp.sum(val * val, axis=1, keepdims=True)
            for b in range(per):
                rows_out.append(to_row(en[b * LANES:(b + 1) * LANES]))
        pad = 8 - len(rows_out)
        esend[c] = jnp.concatenate(rows_out + [jnp.zeros((pad, LANES), f32)], axis=0)
        if c == 0:
            pl.semaphore_wait(barrier, n - 1)
        for d in range(1, n):
            energy_copy(c, d).start()
        if c == 0:
            ld_w[2].wait()
            for cp in ld_kv(0) + ld_h[2:] + [ld_w[3]]:
                cp.start()
            wo_copy.start()
        val = jnp.dot(hid[cs, :], wv[...], preferred_element_type=f32).astype(bf16).astype(f32)
        for h in range(heads):
            vn[h, cs, :] = val[:, h * hd:(h + 1) * hd]

    def norm_rope(c):
        total = esend[c]
        for d in range(1, n):
            energy_copy(c, d).wait_recv()
            total = total + erecv[c, d - 1]
        inv = lax.rsqrt(total / width + NORM_EPS)
        for b in range(per):
            base = c * rc_rows + b * LANES
            rs = pl.ds(base, LANES)
            p = to_col(pos_ref[c * per + b:c * per + b + 1, :].astype(f32)).astype(jnp.int32)
            pcol[rs, :] = jnp.broadcast_to(p, (LANES, LANES))
            hot = jnp.logical_and(lane < 3 * slots, lane % slots == p)
            trig = jnp.dot(jnp.where(hot, 1.0, 0.0).astype(bf16), tab_ref[...], preferred_element_type=f32)
            cos, sin = trig[:, :hd], trig[:, hd:]
            for f, w_ref, which in ((qf, qw_ref, 0), (kf, kw_ref, 1)):
                scale = to_col(inv[which * per + b:which * per + b + 1, :])
                normed = (f[rs, :] * scale * w_ref[...]).astype(bf16).astype(f32)
                rot = []
                for h in range(heads):
                    x = normed[:, h * hd:(h + 1) * hd]
                    rot.append(x * cos + pltpu.roll(x, hd // 2, 1) * sin)
                if which == 0:
                    grouped = jnp.concatenate([r.reshape(LANES // 8, 8, hd) for r in rot], axis=1)
                    qg[pl.ds(base // 8, LANES // 8)] = grouped.astype(bf16)
                else:
                    for h in range(heads):
                        kn[h, rs, :] = rot[h].astype(bf16).astype(f32)

    def attend_block(i, carry):
        base = i * BLK
        n_grp = BLK // 8

        def kv_rows(g, count):
            return pl.ds(pl.multiple_of(base * per_row + g * span, span), count * span)

        for g in range(n_grp):
            s_scr[pl.ds(g * 16, 16), :] = lax.dot_general(
                qg[i * n_grp + g], kc[kv_rows(g, 1), :], (((1,), (1,)), ((), ())), preferred_element_type=f32)
        p_new = []
        for g in range(n_grp):
            r8 = pl.ds(pl.multiple_of(base + g * 8, 8), 8)
            pc = jnp.concatenate([pcol[r8, :]] * heads, axis=0)
            wide_pc = jnp.concatenate([pc] * (span // LANES), axis=1)
            k_own = jnp.concatenate([kn[h, r8, :] for h in range(heads)], axis=0)
            s_own = jnp.sum(qg[i * n_grp + g].astype(f32) * k_own, axis=1, keepdims=True)
            sc = jnp.where(slotm < wide_pc, s_scr[pl.ds(g * 16, 16), :], NEG)
            top = jnp.maximum(jnp.max(sc, axis=1, keepdims=True), s_own)
            e = jnp.exp2((sc - top) * scale2)
            e_own = jnp.exp2((s_own - top) * scale2)
            inv_l = 1.0 / (jnp.sum(e, axis=1, keepdims=True) + e_own)
            p_scr[pl.ds(g * 16, 16), :] = (e * inv_l).astype(bf16)
            p_new.append((e_own * inv_l).astype(bf16).astype(f32))
        for pair in range(n_grp // 2):
            vv = jnp.concatenate([vc[kv_rows(2 * pair, 1), :], vc[kv_rows(2 * pair + 1, 1), :]], axis=1)
            oo = jnp.dot(p_scr[pl.ds(pair * 32, 32), :], vv, preferred_element_type=f32)
            res = []
            for t in range(2):
                g = 2 * pair + t
                r8 = pl.ds(pl.multiple_of(base + g * 8, 8), 8)
                v_own = jnp.concatenate([vn[h, r8, :] for h in range(heads)], axis=0)
                res.append(oo[16 * t:16 * t + 16, t * hd:(t + 1) * hd] + p_new[g] * v_own)
            rs = pl.ds(pl.multiple_of(base + pair * 16, 16), 16)
            for h in range(heads):
                o_scr[rs, h * hd:(h + 1) * hd] = jnp.concatenate(
                    [res[0][8 * h:8 * h + 8], res[1][8 * h:8 * h + 8]], axis=0).astype(bf16)
        return carry

    blocks = rc_rows // BLK

    def attend(c, first, count):
        if first == 0:
            for cp in ld_kv(c):
                cp.wait()
            if c + 1 < nj:
                for cp in ld_kv(c + 1):
                    cp.start()
        lax.fori_loop(c * blocks + first, c * blocks + first + count, attend_block, 0)

    def qs(y, part_no, count):
        return pl.ds(pl.multiple_of(y * own + part_no * hf, hf), count)

    def gs(j, c, y, part_no, count):
        return pl.ds(pl.multiple_of(j * rc_rows + c * half_rows + y * own + part_no * hf, hf), count)

    def remote(kind, j, src, dst, dev):
        return pltpu.make_async_remote_copy(src_ref=src, dst_ref=dst, send_sem=ssem.at[kind, j], recv_sem=rsem.at[kind, j],
                                            device_id={'tp': dev}, device_id_type=MESH)

    sent = []

    def send(kind, j, src, dst, dev):
        cp = remote(kind, j, src, dst, dev)
        cp.start()
        sent.append(cp)

    def recv(kind, j, dst, dev):
        remote(kind, j, dst, dst, dev).wait_recv()

    def p0(j):
        src = pl.ds(pl.multiple_of(j * rc_rows + (1 - core) * half_rows, half_rows), half_rows)
        send(O, j, o_scr.at[src], opart.at[j], mate)

    def p1(j):
        if j == 0:
            ld_w[3].wait()
            wo_copy.wait_recv()
        recv(O, j, opart.at[j], mate)
        mine = o_scr[pl.ds(pl.multiple_of(j * rc_rows + core * half_rows, half_rows), half_rows), :]
        theirs = opart[j]
        step = 512
        for c0 in range(0, width, step):
            acc = jnp.dot(mine, wo[:, c0:c0 + step], preferred_element_type=f32)
            acc = acc + jnp.dot(theirs, wop[:, c0:c0 + step], preferred_element_type=f32)
            part[j, :, c0:c0 + step] = acc.astype(bf16)
        send(A_R, j, part.at[j, qs(xa, 0, hf)], ra.at[j, 0], right)
        send(A_L, j, part.at[j, qs(xa, 1, hf)], ra.at[j, 1], left)
        send(B_R, j, part.at[j, qs(xr, 1, hf)], rb.at[j, 0], right)
        send(B_L, j, part.at[j, qs(xl, 0, hf)], rb.at[j, 1], left)

    def p2(j):
        recv(A_R, j, ra.at[j, 0], left)
        cst[j, 0] = (part[j, qs(xr, 0, hf), :].astype(f32) + ra[j, 0].astype(f32)).astype(bf16)
        send(C_R, j, cst.at[j, 0], rc.at[j, 0], right)
        recv(A_L, j, ra.at[j, 1], right)
        cst[j, 1] = (part[j, qs(xl, 1, hf), :].astype(f32) + ra[j, 1].astype(f32)).astype(bf16)
        send(C_L, j, cst.at[j, 1], rc.at[j, 1], left)

    def p3(j):
        for k in range(2):
            recv((C_R, C_L)[k], j, rc.at[j, k], (left, right)[k])
            recv((B_L, B_R)[k], j, rb.at[j, 1 - k], (right, left)[k])
            a = (part[j, qs(chip, k, hf), :].astype(f32) + rc[j, k].astype(f32) + rb[j, 1 - k].astype(f32))
            inv = lax.rsqrt(jnp.sum(a * a, axis=1, keepdims=True) / width + NORM_EPS)
            mine = gs(j, core, chip, k, hf)
            out_ref[mine, :] = (hid[mine, :].astype(f32) + a * inv * pw_ref[...]).astype(bf16)
        blk = out_ref.at[gs(j, core, chip, 0, own)]
        send(G1_R, j, blk, blk, right)
        send(G1_L, j, blk, blk, left)
        send(D_OWN, j, blk, blk, mate)

    def p4(j):
        bl = out_ref.at[gs(j, core, xl, 0, own)]
        br = out_ref.at[gs(j, core, xr, 0, own)]
        recv(G1_R, j, bl, left)
        fl = out_ref.at[gs(j, core, xl, 0, hf)]
        send(G2_R, j, fl, fl, right)
        send(D_LEFT, j, bl, bl, mate)
        recv(G1_L, j, br, right)
        fr = out_ref.at[gs(j, core, xr, 1, hf)]
        send(G2_L, j, fr, fr, left)
        send(D_RIGHT, j, br, br, mate)

    def p5(j):
        b0 = out_ref.at[gs(j, core, xa, 0, hf)]
        recv(G2_R, j, b0, left)
        send(D_ANT0, j, b0, b0, mate)
        b1 = out_ref.at[gs(j, core, xa, 1, hf)]
        recv(G2_L, j, b1, right)
        send(D_ANT1, j, b1, b1, mate)

    new_out = [pltpu.make_async_copy(kn, kn_hbm, nsem.at[0]), pltpu.make_async_copy(vn, vn_hbm, nsem.at[1])]
    qh, kh = blocks // 2, blocks - blocks // 2
    project_qkv(0)
    project_qkv(1)
    norm_rope(0)
    attend(0, 0, blocks)
    p0(0)
    norm_rope(1)
    p1(0)
    attend(1, 0, qh)
    p2(0)
    attend(1, qh, kh)
    p0(1)
    project_qkv(2)
    p1(1)
    p3(0)
    norm_rope(2)
    attend(2, 0, qh)
    p2(1)
    p4(0)
    attend(2, qh, kh)
    p0(2)
    project_qkv(3)
    p1(2)
    p3(1)
    p5(0)
    norm_rope(3)
    for cp in new_out:
        cp.start()
    attend(3, 0, qh)
    p2(2)
    p4(1)
    attend(3, qh, kh)
    p0(3)
    p1(3)
    p3(2)
    p5(1)
    p2(3)
    p4(2)
    p3(3)
    p5(2)
    p4(3)
    p5(3)
    for j in range(nj):
        oc = 1 - core
        recv(D_OWN, j, out_ref.at[gs(j, oc, chip, 0, own)], mate)
        recv(D_LEFT, j, out_ref.at[gs(j, oc, xl, 0, own)], mate)
        recv(D_RIGHT, j, out_ref.at[gs(j, oc, xr, 0, own)], mate)
        recv(D_ANT0, j, out_ref.at[gs(j, oc, xa, 0, hf)], mate)
        recv(D_ANT1, j, out_ref.at[gs(j, oc, xa, 1, hf)], mate)
    for cp in sent:
        cp.wait_send()
    for c in range(nj):
        for d in range(1, n):
            energy_copy(c, d).wait_send()
    wo_copy.wait_send()
    for cp in new_out:
        cp.wait()


def decode_step(n, slots, heads, hd, positions, hidden, w_q, w_k, w_v, w_o, q_norm_w, k_norm_w, post_norm_w, k_flat, v_flat, nj=4):
    rows, width = hidden.shape
    cols = heads * hd
    rc_rows = rows // nj
    half = rc_rows // 2
    own = half // (n // 2)
    hf = own // 2
    span = 8 * slots * heads
    f32, bf16 = jnp.float32, jnp.bfloat16
    dma = pltpu.SemaphoreType.DMA
    return pl.pallas_call(
        functools.partial(step_kernel, n, nj, slots, heads, hd),
        out_shape=(pltpu.VMEM(k_flat.shape, bf16), pltpu.VMEM(v_flat.shape, bf16), pltpu.VMEM((rows, width), bf16),
                   jax.ShapeDtypeStruct((heads, rows, hd), f32), jax.ShapeDtypeStruct((heads, rows, hd), f32)),
        in_specs=[VMEM_SPEC] * 5 + [HBM_SPEC] * 7,
        out_specs=(VMEM_SPEC,) * 3 + (HBM_SPEC,) * 2,
        scratch_shapes=[
            pltpu.VMEM((heads, rows, hd), f32), pltpu.VMEM((heads, rows, hd), f32),
            pltpu.VMEM((rows, width), bf16), pltpu.VMEM((width, cols), bf16), pltpu.VMEM((width, cols), bf16),
            pltpu.VMEM((width, cols), bf16), pltpu.VMEM((cols, width), bf16), pltpu.VMEM((cols, width), bf16),
            pltpu.VMEM((rows, cols), f32), pltpu.VMEM((rows, cols), f32), pltpu.VMEM((rows // 8, 8 * heads, hd), bf16),
            pltpu.VMEM((rows, LANES), jnp.int32), pltpu.VMEM((BLK * heads, span), f32), pltpu.VMEM((BLK * heads, span), bf16),
            pltpu.VMEM((rows, cols), bf16), pltpu.VMEM((nj, half, cols), bf16), pltpu.VMEM((nj, half, width), bf16),
            pltpu.VMEM((nj, 2, hf, width), bf16), pltpu.VMEM((nj, 2, hf, width), bf16),
            pltpu.VMEM((nj, 2, hf, width), bf16), pltpu.VMEM((nj, 2, hf, width), bf16),
            pltpu.VMEM((nj, 8, LANES), f32), pltpu.VMEM((nj, n - 1, 8, LANES), f32),
            dma((4 + nj,)), dma((2, nj)), dma((2,)), dma((2,)), dma((nj, n - 1)), dma((nj, n - 1)), dma((16, nj)), dma((16, nj)),
        ],
        compiler_params=pltpu.CompilerParams(collective_id=0, has_side_effects=True, vmem_limit_bytes=26 << 20),
        name='decode_step',
    )(positions.reshape(rows // LANES, LANES), jnp.asarray(rope_table(slots, hd)), q_norm_w.reshape(1, cols),
      k_norm_w.reshape(1, cols), post_norm_w.reshape(1, width), hidden, w_q, w_k, w_v, w_o, k_flat, v_flat)


def store_kernel(blk, slots, heads, hd, pos_s, kn, vn, kc, vc, ko, vo, kc_alias, vc_alias, mtab, sem):
    rows = kn.shape[1]
    per_row = slots * heads
    even = lax.broadcasted_iota(jnp.int32, (8, hd), 0) % heads == 0
    pair_id = lax.broadcasted_iota(jnp.int32, (8, hd), 0) // heads
    for k in range(4):
        mtab[k] = jnp.where(pair_id == k, 1.0, 0.0).astype(jnp.bfloat16)

    def copies(i):
        sl = pl.ds(pl.multiple_of(i * blk * per_row, blk * per_row), blk * per_row)
        return [pltpu.make_async_copy(kc_alias.at[sl], ko.at[sl], sem.at[0, i]),
                pltpu.make_async_copy(vc_alias.at[sl], vo.at[sl], sem.at[1, i])]

    def body(i, carry):
        base = i * blk
        for r in range(blk):
            p = pos_s[base + r]
            at = pl.ds(pl.multiple_of((base + r) * per_row + lax.shift_left(lax.shift_right_logical(p, 2), 3), 8), 8)
            hit = mtab[p & 3] > 0
            row = pl.ds(base + r, 8, stride=0)
            for src, dst in ((kn, kc_alias), (vn, vc_alias)):
                new = jnp.where(even, src[0, row, :], src[1, row, :]).astype(jnp.bfloat16)
                dst[at, :] = jnp.where(hit, new, dst[at, :])
        for cp in copies(i):
            cp.start()
        return carry

    lax.fori_loop(0, rows // blk, body, 0)
    for i in range(rows // blk):
        for cp in copies(i):
            cp.wait()


def store(positions, kn, vn, k_vm, v_vm, slots, heads, hd, blk=64):
    rows = kn.shape[1]
    bf16 = jnp.bfloat16
    dma = pltpu.SemaphoreType.DMA
    res = pl.pallas_call(
        functools.partial(store_kernel, blk, slots, heads, hd),
        out_shape=(jax.ShapeDtypeStruct(k_vm.shape, bf16),
                   jax.ShapeDtypeStruct(v_vm.shape, bf16), pltpu.VMEM(k_vm.shape, bf16), pltpu.VMEM(v_vm.shape, bf16)),
        in_specs=[pl.BlockSpec(memory_space=pltpu.SMEM)] + [VMEM_SPEC] * 4,
        out_specs=(HBM_SPEC, HBM_SPEC, VMEM_SPEC, VMEM_SPEC),
        input_output_aliases={3: 2, 4: 3},
        scratch_shapes=[pltpu.VMEM((4, 8, hd), bf16), dma((2, rows // blk))],
        compiler_params=pltpu.CompilerParams(vmem_limit_bytes=26 << 20),
        name='store',
    )(positions, kn, vn, k_vm, v_vm)
    return res[:2]


def solution(mesh):
    n = mesh.shape['tp']

    def local_step(hidden, w_q, w_k, w_v, w_o, q_norm_w, k_norm_w, post_norm_w, k_cache, v_cache, positions):
        rows, slots, heads, hd = k_cache.shape
        flat = (rows * slots * heads, hd)
        k_vm, v_vm, hid_vm, kn, vn = decode_step(n, slots, heads, hd, positions, hidden, w_q, w_k, w_v, w_o, q_norm_w,
                                                 k_norm_w, post_norm_w, k_cache.reshape(flat), v_cache.reshape(flat))
        k_new, v_new = store(positions, kn, vn, k_vm, v_vm, slots, heads, hd)
        return hid_vm, k_new.reshape(k_cache.shape), v_new.reshape(v_cache.shape)

    cache_spec = P('dp', None, 'tp', None)
    return jax.shard_map(local_step, mesh=mesh, in_specs=(P('dp', None), P(None, 'tp'), P(None, 'tp'), P(None, 'tp'), P('tp', None), P('tp'), P('tp'), P(None), cache_spec, cache_spec, P('dp')), out_specs=(P('dp', None), cache_spec, cache_spec), check_vma=False)
```

```python
import functools
import math

import jax
import jax.numpy as jnp
import numpy as np
from jax import lax
from jax.experimental import pallas as pl
from jax.experimental.pallas import tpu as pltpu
from jax.sharding import PartitionSpec as P

NORM_EPS = 1e-6
ROPE_BASE = 500000.0
NEG = -1e30
MESH = pl.DeviceIdType.MESH
VMEM_SPEC = pl.BlockSpec(memory_space=pltpu.VMEM)
HBM_SPEC = pl.BlockSpec(memory_space=pltpu.HBM)
LANES = 128
BLK = 128
CHUNKS = (2, 2, 2, 2)
ORDER = (
         'Q0', 'Q1', 'R0', 'T0.0', 'T0.1', 'a0', 'R1', 'b0', 'T1.0', 'T1.1', 'a1', 'Q2',
         'c0', 'b1', 'Q3', 'R2', 'T2.0', 'd0', 'T2.1', 'c1', 'a2', 'R3', 'b2', 'T3.0',
         'T3.1', 'e0', 'a3', 'b3', 'c2', 'f0', 'd1', 'c3', 'd2', 'e1', 'd3', 'e2',
         'e3', 'f1', 'f2', 'f3',
)


def rope_table(slots, head_dim):
    half = head_dim // 2
    inv_freq = np.float32(ROPE_BASE) ** (np.float32(-2.0) * np.arange(half, dtype=np.float32) / np.float32(head_dim))
    angles = (np.arange(slots, dtype=np.float32)[:, None] * inv_freq[None, :].astype(np.float32)).astype(np.float64)
    cos, sin = np.cos(angles).astype(np.float32), np.sin(angles).astype(np.float32)
    full = np.concatenate([cos, cos, -sin, sin], axis=1)
    parts, rest = [], full
    for _ in range(3):
        part = rest.astype(jnp.bfloat16)
        parts.append(part)
        rest = rest - part.astype(np.float32)
    pad = np.zeros((LANES - 3 * slots, full.shape[1]), jnp.bfloat16)
    return np.concatenate(parts + [pad], axis=0)


(O, A_R, A_L, B_R, B_L, C_R, C_L, G1_R0, G1_R1, G1_L0, G1_L1, G2_R, G2_L,
 D_OWN, D_LEFT, D_RIGHT, D_ANT0, D_ANT1) = range(18)


def step_kernel(n, sizes, slots, heads, hd,
                pos_hbm, tab_hbm, qw_hbm, kw_hbm, pw_hbm, hid_hbm, wq_hbm, wk_hbm, wv_hbm, wo_hbm, kc_hbm, vc_hbm,
                kc, vc, out_ref, kn_hbm, vn_hbm,
                kn, vn, pos_ref, tab_ref, qw_ref, kw_ref, pw_ref, hid, wq, wk, wv, wo, wop, qf, kf, qg, pcol, s_scr, p_scr, o_scr, opart, part, ra, rb, rc, cst,
                esend, erecv, lsem, psem, csem, nsem, osem, essem, ersem, ssem, rsem):
    me = lax.axis_index('tp')
    rows, width = hid_hbm.shape
    cols = heads * hd
    per_row = slots * heads
    nj = len(sizes)
    starts = [sum(sizes[:j]) for j in range(nj)]
    nchip = n // 2
    chip, core = me // 2, lax.rem(me, 2)
    half_of = [r // 2 for r in sizes]
    own_of = [r // n for r in sizes]
    hf_of = [r // (2 * n) for r in sizes]
    xr, xl, xa = lax.rem(chip + 1, nchip), lax.rem(chip + nchip - 1, nchip), lax.rem(chip + 2, nchip)
    right, left, mate = xr * 2 + core, xl * 2 + core, chip * 2 + (1 - core)
    f32, bf16 = jnp.float32, jnp.bfloat16

    def chunk(c):
        return pl.ds(starts[c], sizes[c])

    ld_w = [pltpu.make_async_copy(src, dst, lsem.at[k]) for k, (src, dst) in
            enumerate(((wq_hbm, wq), (wk_hbm, wk), (wv_hbm, wv), (wo_hbm, wo)))]
    ld_h = [pltpu.make_async_copy(hid_hbm.at[chunk(c)], hid.at[chunk(c)], lsem.at[4 + c]) for c in range(nj)]

    def ld_kv(c):
        sl = pl.ds(starts[c] * per_row, sizes[c] * per_row)
        return [pltpu.make_async_copy(kc_hbm.at[sl], kc.at[sl], csem.at[0, c]),
                pltpu.make_async_copy(vc_hbm.at[sl], vc.at[sl], csem.at[1, c])]

    ld_p = [pltpu.make_async_copy(src, dst, psem.at[k]) for k, (src, dst) in enumerate(
        ((pos_hbm, pos_ref), (tab_hbm, tab_ref), (qw_hbm, qw_ref), (kw_hbm, kw_ref), (pw_hbm, pw_ref)))]
    for cp in [ld_h[0], ld_w[0], ld_w[1]] + ld_p + [ld_w[2], ld_h[1]]:
        cp.start()

    barrier = pltpu.get_barrier_semaphore()
    for d in range(1, n):
        pl.semaphore_signal(barrier, inc=1, device_id={'tp': lax.rem(me + d, n)}, device_id_type=MESH)

    lane = lax.broadcasted_iota(jnp.int32, (LANES, LANES), 1)
    sub = lax.broadcasted_iota(jnp.int32, (LANES, LANES), 0)
    eye = lane == sub
    span = 8 * per_row
    ci = lax.broadcasted_iota(jnp.int32, (16, span), 1)
    ri = lax.broadcasted_iota(jnp.int32, (16, span), 0)
    match = jnp.logical_and(ci // per_row == ri % 8, ci % heads == ri // 8)
    slotm = jnp.where(match, (ci % per_row) // heads, 1000)
    scale2 = (hd ** -0.5) * math.log2(math.e)

    def to_row(col):
        return jnp.sum(jnp.where(eye, jnp.broadcast_to(col, (LANES, LANES)), 0.0), axis=0, keepdims=True)

    def to_col(row):
        return jnp.sum(jnp.where(eye, jnp.broadcast_to(row, (LANES, LANES)), 0.0), axis=1, keepdims=True)

    def energy_copy(c, d):
        return pltpu.make_async_remote_copy(
            src_ref=esend.at[c], dst_ref=erecv.at[c, d - 1], send_sem=essem.at[c, d - 1], recv_sem=ersem.at[c, d - 1],
            device_id={'tp': lax.rem(me + d, n)}, device_id_type=MESH)

    wo_copy = pltpu.make_async_remote_copy(
        src_ref=wo_hbm, dst_ref=wop, send_sem=osem.at[0], recv_sem=osem.at[1],
        device_id={'tp': mate}, device_id_type=MESH)

    def project_qkv(c):
        cs, per = chunk(c), sizes[c] // LANES
        ld_h[c].wait()
        rows_out = []
        for k, (w, f) in enumerate(((wq, qf), (wk, kf))):
            if c == 0:
                ld_w[k].wait()
            val = jnp.dot(hid[cs, :], w[...], preferred_element_type=f32).astype(bf16).astype(f32)
            f[cs, :] = val
            en = jnp.sum(val * val, axis=1, keepdims=True)
            for b in range(per):
                rows_out.append(to_row(en[b * LANES:(b + 1) * LANES]))
            if c == 0 and k == 1:
                for cp in ld_h[2:4] + ld_kv(0) + ld_kv(1) + ld_h[4:] + [ld_w[3]]:
                    cp.start()
        pad = 8 - len(rows_out)
        esend[c] = jnp.concatenate(rows_out + [jnp.zeros((pad, LANES), f32)], axis=0)
        if c == 0:
            pl.semaphore_wait(barrier, n - 1)
        for d in range(1, n):
            energy_copy(c, d).start()
        if c == 0:
            ld_w[2].wait()
            wo_copy.start()
        if 0 < c < nj - 1:
            for cp in ld_kv(c + 1):
                cp.start()
        val = jnp.dot(hid[cs, :], wv[...], preferred_element_type=f32).astype(bf16).astype(f32)
        for h in range(heads):
            vn[h, cs, :] = val[:, h * hd:(h + 1) * hd]

    def norm_rope(c):
        if c == 0:
            for cp in ld_p:
                cp.wait()
        total, per = esend[c], sizes[c] // LANES
        for d in range(1, n):
            energy_copy(c, d).wait_recv()
            total = total + erecv[c, d - 1]
        inv = lax.rsqrt(total / width + NORM_EPS)
        for b in range(per):
            base = starts[c] + b * LANES
            rs = pl.ds(base, LANES)
            p = to_col(pos_ref[starts[c] // LANES + b:starts[c] // LANES + b + 1, :].astype(f32)).astype(jnp.int32)
            pcol[rs, :] = jnp.broadcast_to(p, (LANES, LANES))
            hot = jnp.logical_and(lane < 3 * slots, lane % slots == p)
            trig = jnp.dot(jnp.where(hot, 1.0, 0.0).astype(bf16), tab_ref[...], preferred_element_type=f32)
            cos, sin = trig[:, :hd], trig[:, hd:]
            for f, w_ref, which in ((qf, qw_ref, 0), (kf, kw_ref, 1)):
                scale = to_col(inv[which * per + b:which * per + b + 1, :])
                normed = (f[rs, :] * scale * w_ref[...]).astype(bf16).astype(f32)
                rot = []
                for h in range(heads):
                    x = normed[:, h * hd:(h + 1) * hd]
                    rot.append(x * cos + pltpu.roll(x, hd // 2, 1) * sin)
                if which == 0:
                    grouped = jnp.concatenate([r.reshape(LANES // 8, 8, hd) for r in rot], axis=1)
                    qg[pl.ds(base // 8, LANES // 8)] = grouped.astype(bf16)
                else:
                    for h in range(heads):
                        kn[h, rs, :] = rot[h].astype(bf16).astype(f32)

    def attend_block(i, carry):
        base = i * BLK
        n_grp = BLK // 8

        def kv_rows(g, count):
            return pl.ds(pl.multiple_of(base * per_row + g * span, span), count * span)

        for g in range(n_grp):
            s_scr[pl.ds(g * 16, 16), :] = lax.dot_general(
                qg[i * n_grp + g], kc[kv_rows(g, 1), :], (((1,), (1,)), ((), ())), preferred_element_type=f32)
        p_new = []
        for g in range(n_grp):
            r8 = pl.ds(pl.multiple_of(base + g * 8, 8), 8)
            pc = jnp.concatenate([pcol[r8, :]] * heads, axis=0)
            wide_pc = jnp.concatenate([pc] * (span // LANES), axis=1)
            k_own = jnp.concatenate([kn[h, r8, :] for h in range(heads)], axis=0)
            s_own = jnp.sum(qg[i * n_grp + g].astype(f32) * k_own, axis=1, keepdims=True)
            sc = jnp.where(slotm < wide_pc, s_scr[pl.ds(g * 16, 16), :], NEG)
            top = jnp.maximum(jnp.max(sc, axis=1, keepdims=True), s_own)
            e = jnp.exp2((sc - top) * scale2)
            e_own = jnp.exp2((s_own - top) * scale2)
            inv_l = 1.0 / (jnp.sum(e, axis=1, keepdims=True) + e_own)
            p_scr[pl.ds(g * 16, 16), :] = (e * inv_l).astype(bf16)
            p_new.append((e_own * inv_l).astype(bf16).astype(f32))
        for pair in range(n_grp // 2):
            vv = jnp.concatenate([vc[kv_rows(2 * pair, 1), :], vc[kv_rows(2 * pair + 1, 1), :]], axis=1)
            oo = jnp.dot(p_scr[pl.ds(pair * 32, 32), :], vv, preferred_element_type=f32)
            res = []
            for t in range(2):
                g = 2 * pair + t
                r8 = pl.ds(pl.multiple_of(base + g * 8, 8), 8)
                v_own = jnp.concatenate([vn[h, r8, :] for h in range(heads)], axis=0)
                res.append(oo[16 * t:16 * t + 16, t * hd:(t + 1) * hd] + p_new[g] * v_own)
            rs = pl.ds(pl.multiple_of(base + pair * 16, 16), 16)
            for h in range(heads):
                o_scr[rs, h * hd:(h + 1) * hd] = jnp.concatenate(
                    [res[0][8 * h:8 * h + 8], res[1][8 * h:8 * h + 8]], axis=0).astype(bf16)
        return carry

    def attend(c, piece):
        if piece == 0:
            for cp in ld_kv(c):
                cp.wait()
        first = (starts[c] + piece * LANES) // BLK
        lax.fori_loop(first, first + LANES // BLK, attend_block, 0)

    def mine_of(j):
        return pl.ds(starts[j] // 2, half_of[j])

    def fs(j):
        return pl.ds(starts[j] // (2 * n), hf_of[j])

    def qs(j, y, part_no):
        return pl.ds(pl.multiple_of(starts[j] // 2 + y * own_of[j] + part_no * hf_of[j], hf_of[j]), hf_of[j])

    def os(j, c):
        return pl.ds(pl.multiple_of(starts[j] + c * half_of[j], half_of[j]), half_of[j])

    def gs(j, c, y, part_no=None):
        first = starts[j] + c * half_of[j] + y * own_of[j]
        if part_no is None:
            return pl.ds(pl.multiple_of(first, own_of[j]), own_of[j])
        return pl.ds(pl.multiple_of(first + part_no * hf_of[j], hf_of[j]), hf_of[j])

    def remote(kind, j, src, dst, dev):
        return pltpu.make_async_remote_copy(src_ref=src, dst_ref=dst, send_sem=ssem.at[kind, j], recv_sem=rsem.at[kind, j],
                                            device_id={'tp': dev}, device_id_type=MESH)

    sent = []

    def send(kind, j, src, dst, dev):
        cp = remote(kind, j, src, dst, dev)
        cp.start()
        sent.append(cp)

    def recv(kind, j, dst, dev):
        remote(kind, j, dst, dst, dev).wait_recv()

    def p0(j):
        send(O, j, o_scr.at[os(j, 1 - core)], opart.at[mine_of(j)], mate)

    def p1(j):
        if j == 0:
            ld_w[3].wait()
            wo_copy.wait_recv()
        recv(O, j, opart.at[mine_of(j)], mate)
        mine = o_scr[os(j, core), :]
        theirs = opart[mine_of(j), :]
        step = 512
        for c0 in range(0, width, step):
            acc = jnp.dot(mine, wo[:, c0:c0 + step], preferred_element_type=f32)
            acc = acc + jnp.dot(theirs, wop[:, c0:c0 + step], preferred_element_type=f32)
            part[mine_of(j), c0:c0 + step] = acc.astype(bf16)
        send(A_R, j, part.at[qs(j, xa, 0)], ra.at[0, fs(j)], right)
        send(A_L, j, part.at[qs(j, xa, 1)], ra.at[1, fs(j)], left)
        send(B_R, j, part.at[qs(j, xr, 1)], rb.at[0, fs(j)], right)
        send(B_L, j, part.at[qs(j, xl, 0)], rb.at[1, fs(j)], left)

    def p2(j):
        for k in range(2):
            recv((A_R, A_L)[k], j, ra.at[k, fs(j)], (left, right)[k])
            own_part = part[qs(j, (xr, xl)[k], k), :].astype(f32)
            cst[k, fs(j), :] = (own_part + ra[k, fs(j), :].astype(f32)).astype(bf16)
            send((C_R, C_L)[k], j, cst.at[k, fs(j)], rc.at[k, fs(j)], (right, left)[k])

    def p3(j):
        for k in range(2):
            recv((B_L, B_R)[k], j, rb.at[1 - k, fs(j)], (right, left)[k])
            recv((C_R, C_L)[k], j, rc.at[k, fs(j)], (left, right)[k])
            a = (part[qs(j, chip, k), :].astype(f32) + rc[k, fs(j), :].astype(f32) + rb[1 - k, fs(j), :].astype(f32))
            inv = lax.rsqrt(jnp.sum(a * a, axis=1, keepdims=True) / width + NORM_EPS)
            mine = gs(j, core, chip, k)
            out_ref[mine, :] = (hid[mine, :].astype(f32) + a * inv * pw_ref[...]).astype(bf16)
        blk = out_ref.at[gs(j, core, chip)]
        h0, h1 = out_ref.at[gs(j, core, chip, 0)], out_ref.at[gs(j, core, chip, 1)]
        send(G1_R0, j, h0, h0, right)
        send(G1_L1, j, h1, h1, left)
        send(G1_R1, j, h1, h1, right)
        send(G1_L0, j, h0, h0, left)
        send(D_OWN, j, blk, blk, mate)

    def p4(j):
        bl = [out_ref.at[gs(j, core, xl, k)] for k in range(2)]
        br = [out_ref.at[gs(j, core, xr, k)] for k in range(2)]
        recv(G1_R0, j, bl[0], left)
        send(G2_R, j, bl[0], bl[0], right)
        recv(G1_L1, j, br[1], right)
        send(G2_L, j, br[1], br[1], left)
        recv(G1_R1, j, bl[1], left)
        full_l = out_ref.at[gs(j, core, xl)]
        send(D_LEFT, j, full_l, full_l, mate)
        recv(G1_L0, j, br[0], right)
        full_r = out_ref.at[gs(j, core, xr)]
        send(D_RIGHT, j, full_r, full_r, mate)

    def p5(j):
        b0 = out_ref.at[gs(j, core, xa, 0)]
        recv(G2_R, j, b0, left)
        send(D_ANT0, j, b0, b0, mate)
        b1 = out_ref.at[gs(j, core, xa, 1)]
        recv(G2_L, j, b1, right)
        send(D_ANT1, j, b1, b1, mate)

    new_out = [pltpu.make_async_copy(kn, kn_hbm, nsem.at[0]), pltpu.make_async_copy(vn, vn_hbm, nsem.at[1])]
    stages = dict(Q=project_qkv, R=norm_rope, T=attend, a=p0, b=p1, c=p2, d=p3, e=p4, f=p5)
    for token in ORDER:
        stages[token[0]](*map(int, token[1:].split('.')))
        if token == 'R' + str(nj - 1):
            for cp in new_out:
                cp.start()
    for j in range(nj):
        oc = 1 - core
        recv(D_OWN, j, out_ref.at[gs(j, oc, chip)], mate)
        recv(D_LEFT, j, out_ref.at[gs(j, oc, xl)], mate)
        recv(D_RIGHT, j, out_ref.at[gs(j, oc, xr)], mate)
        recv(D_ANT0, j, out_ref.at[gs(j, oc, xa, 0)], mate)
        recv(D_ANT1, j, out_ref.at[gs(j, oc, xa, 1)], mate)
    for cp in sent:
        cp.wait_send()
    for c in range(nj):
        for d in range(1, n):
            energy_copy(c, d).wait_send()
    wo_copy.wait_send()
    for cp in new_out:
        cp.wait()


def decode_step(n, slots, heads, hd, positions, hidden, w_q, w_k, w_v, w_o, q_norm_w, k_norm_w, post_norm_w, k_flat, v_flat, sizes):
    rows, width = hidden.shape
    cols = heads * hd
    nj = len(sizes)
    span = 8 * slots * heads
    f32, bf16 = jnp.float32, jnp.bfloat16
    dma = pltpu.SemaphoreType.DMA
    return pl.pallas_call(
        functools.partial(step_kernel, n, sizes, slots, heads, hd),
        out_shape=(pltpu.VMEM(k_flat.shape, bf16), pltpu.VMEM(v_flat.shape, bf16), pltpu.VMEM((rows, width), bf16),
                   jax.ShapeDtypeStruct((heads, rows, hd), f32), jax.ShapeDtypeStruct((heads, rows, hd), f32)),
        in_specs=[HBM_SPEC] * 12,
        out_specs=(VMEM_SPEC,) * 3 + (HBM_SPEC,) * 2,
        scratch_shapes=[
            pltpu.VMEM((heads, rows, hd), f32), pltpu.VMEM((heads, rows, hd), f32),
            pltpu.VMEM((rows // LANES, LANES), jnp.int32), pltpu.VMEM((LANES, 2 * hd), bf16), pltpu.VMEM((1, cols), f32),
            pltpu.VMEM((1, cols), f32), pltpu.VMEM((1, width), f32),
            pltpu.VMEM((rows, width), bf16), pltpu.VMEM((width, cols), bf16), pltpu.VMEM((width, cols), bf16),
            pltpu.VMEM((width, cols), bf16), pltpu.VMEM((cols, width), bf16), pltpu.VMEM((cols, width), bf16),
            pltpu.VMEM((rows, cols), f32), pltpu.VMEM((rows, cols), f32), pltpu.VMEM((rows // 8, 8 * heads, hd), bf16),
            pltpu.VMEM((rows, LANES), jnp.int32), pltpu.VMEM((BLK * heads, span), f32), pltpu.VMEM((BLK * heads, span), bf16),
            pltpu.VMEM((rows, cols), bf16), pltpu.VMEM((rows // 2, cols), bf16), pltpu.VMEM((rows // 2, width), bf16),
            pltpu.VMEM((2, rows // (2 * n), width), bf16), pltpu.VMEM((2, rows // (2 * n), width), bf16),
            pltpu.VMEM((2, rows // (2 * n), width), bf16), pltpu.VMEM((2, rows // (2 * n), width), bf16),
            pltpu.VMEM((nj, 8, LANES), f32), pltpu.VMEM((nj, n - 1, 8, LANES), f32),
            dma((4 + nj,)), dma((5,)), dma((2, nj)), dma((2,)), dma((2,)), dma((nj, n - 1)), dma((nj, n - 1)), dma((18, nj)), dma((18, nj)),
        ],
        compiler_params=pltpu.CompilerParams(collective_id=0, has_side_effects=True, vmem_limit_bytes=26 << 20),
        name='decode_step',
    )(positions.reshape(rows // LANES, LANES), jnp.asarray(rope_table(slots, hd)), q_norm_w.reshape(1, cols),
      k_norm_w.reshape(1, cols), post_norm_w.reshape(1, width), hidden, w_q, w_k, w_v, w_o, k_flat, v_flat)


def store_kernel(blk, slots, heads, hd, pos_s, kn, vn, kc, vc, ko, vo, kc_alias, vc_alias, mtab, sem):
    rows = kn.shape[1]
    per_row = slots * heads
    even = lax.broadcasted_iota(jnp.int32, (8, hd), 0) % heads == 0
    pair_id = lax.broadcasted_iota(jnp.int32, (8, hd), 0) // heads
    for k in range(4):
        mtab[k] = jnp.where(pair_id == k, 1.0, 0.0).astype(jnp.bfloat16)

    def copies(i):
        sl = pl.ds(pl.multiple_of(i * blk * per_row, blk * per_row), blk * per_row)
        return [pltpu.make_async_copy(kc_alias.at[sl], ko.at[sl], sem.at[0, i]),
                pltpu.make_async_copy(vc_alias.at[sl], vo.at[sl], sem.at[1, i])]

    def body(i, carry):
        base = i * blk
        for r in range(blk):
            p = pos_s[base + r]
            at = pl.ds(pl.multiple_of((base + r) * per_row + lax.shift_left(lax.shift_right_logical(p, 2), 3), 8), 8)
            hit = mtab[p & 3] > 0
            row = pl.ds(base + r, 8, stride=0)
            for src, dst in ((kn, kc_alias), (vn, vc_alias)):
                new = jnp.where(even, src[0, row, :], src[1, row, :]).astype(jnp.bfloat16)
                dst[at, :] = jnp.where(hit, new, dst[at, :])
        for cp in copies(i):
            cp.start()
        return carry

    lax.fori_loop(0, rows // blk, body, 0)
    for i in range(rows // blk):
        for cp in copies(i):
            cp.wait()


def store(positions, kn, vn, k_vm, v_vm, slots, heads, hd, blk=64):
    rows = kn.shape[1]
    bf16 = jnp.bfloat16
    dma = pltpu.SemaphoreType.DMA
    res = pl.pallas_call(
        functools.partial(store_kernel, blk, slots, heads, hd),
        out_shape=(jax.ShapeDtypeStruct(k_vm.shape, bf16),
                   jax.ShapeDtypeStruct(v_vm.shape, bf16), pltpu.VMEM(k_vm.shape, bf16), pltpu.VMEM(v_vm.shape, bf16)),
        in_specs=[pl.BlockSpec(memory_space=pltpu.SMEM)] + [VMEM_SPEC] * 4,
        out_specs=(HBM_SPEC, HBM_SPEC, VMEM_SPEC, VMEM_SPEC),
        input_output_aliases={3: 2, 4: 3},
        scratch_shapes=[pltpu.VMEM((4, 8, hd), bf16), dma((2, rows // blk))],
        compiler_params=pltpu.CompilerParams(vmem_limit_bytes=26 << 20),
        name='store',
    )(positions, kn, vn, k_vm, v_vm)
    return res[:2]


def chunk_sizes(rows):
    unit = rows // 8
    return [unit * k for k in CHUNKS]


def solution(mesh):
    n = mesh.shape['tp']

    def local_step(hidden, w_q, w_k, w_v, w_o, q_norm_w, k_norm_w, post_norm_w, k_cache, v_cache, positions):
        rows, slots, heads, hd = k_cache.shape
        flat = (rows * slots * heads, hd)
        k_vm, v_vm, hid_vm, kn, vn = decode_step(n, slots, heads, hd, positions, hidden, w_q, w_k, w_v, w_o, q_norm_w,
                                                 k_norm_w, post_norm_w, k_cache.reshape(flat), v_cache.reshape(flat), chunk_sizes(rows))
        k_new, v_new = store(positions, kn, vn, k_vm, v_vm, slots, heads, hd)
        return hid_vm, k_new.reshape(k_cache.shape), v_new.reshape(v_cache.shape)

    cache_spec = P('dp', None, 'tp', None)
    return jax.shard_map(local_step, mesh=mesh, in_specs=(P('dp', None), P(None, 'tp'), P(None, 'tp'), P(None, 'tp'), P('tp', None), P('tp'), P('tp'), P(None), cache_spec, cache_spec, P('dp')), out_specs=(P('dp', None), cache_spec, cache_spec), check_vma=False)
```

```python
import functools
import math

import jax
import jax.numpy as jnp
import numpy as np
from jax import lax
from jax.experimental import pallas as pl
from jax.experimental.pallas import tpu as pltpu
from jax.sharding import PartitionSpec as P

NORM_EPS = 1e-6
ROPE_BASE = 500000.0
NEG = -1e30
MESH = pl.DeviceIdType.MESH
VMEM_SPEC = pl.BlockSpec(memory_space=pltpu.VMEM)
HBM_SPEC = pl.BlockSpec(memory_space=pltpu.HBM)
LANES = 128
BLK = 128
CHUNKS = (2, 2, 2, 2)
ORDER = (
         'Q0', 'Q1', 'R0', 'T0.0', 'T0.1', 'a0', 'R1', 'b0', 'T1.0', 'T1.1', 'a1', 'Q2',
         'c0', 'b1', 'Q3', 'R2', 'T2.0', 'd0', 'T2.1', 'c1', 'a2', 'R3', 'b2', 'T3.0',
         'T3.1', 'e0', 'a3', 'b3', 'c2', 'f0', 'd1', 'c3', 'd2', 'e1', 'd3', 'e2',
         'f1', 'e3', 'f2', 'f3',
)


def rope_table(slots, head_dim):
    half = head_dim // 2
    inv_freq = np.float32(ROPE_BASE) ** (np.float32(-2.0) * np.arange(half, dtype=np.float32) / np.float32(head_dim))
    angles = (np.arange(slots, dtype=np.float32)[:, None] * inv_freq[None, :].astype(np.float32)).astype(np.float64)
    cos, sin = np.cos(angles).astype(np.float32), np.sin(angles).astype(np.float32)
    full = np.concatenate([cos, cos, -sin, sin], axis=1)
    parts, rest = [], full
    for _ in range(3):
        part = rest.astype(jnp.bfloat16)
        parts.append(part)
        rest = rest - part.astype(np.float32)
    pad = np.zeros((LANES - 3 * slots, full.shape[1]), jnp.bfloat16)
    return np.concatenate(parts + [pad], axis=0)


(O, A_R, A_L, B_R, B_L, C_R, C_L, G1_R0, G1_R1, G1_L0, G1_L1, G2_R, G2_L,
 D_OWN, D_LEFT, D_RIGHT, D_ANT0, D_ANT1) = range(18)


def step_kernel(n, sizes, slots, heads, hd,
                pos_hbm, tab_hbm, qw_hbm, kw_hbm, pw_hbm, hid_hbm, wq_hbm, wk_hbm, wv_hbm, wo_hbm, kc_hbm, vc_hbm,
                kc, vc, out_ref, kn_hbm, vn_hbm,
                kn, vn, pos_ref, tab_ref, qw_ref, kw_ref, pw_ref, hid, wq, wk, wv, wo, wop, qf, kf, qg, pcol, s_scr, p_scr, o_scr, opart, part, ra, rb, rc, cst,
                esend, erecv, lsem, psem, csem, nsem, osem, essem, ersem, ssem, rsem):
    me = lax.axis_index('tp')
    rows, width = hid_hbm.shape
    cols = heads * hd
    per_row = slots * heads
    nj = len(sizes)
    starts = [sum(sizes[:j]) for j in range(nj)]
    nchip = n // 2
    chip, core = me // 2, lax.rem(me, 2)
    half_of = [r // 2 for r in sizes]
    own_of = [r // n for r in sizes]
    hf_of = [r // (2 * n) for r in sizes]
    xr, xl, xa = lax.rem(chip + 1, nchip), lax.rem(chip + nchip - 1, nchip), lax.rem(chip + 2, nchip)
    right, left, mate = xr * 2 + core, xl * 2 + core, chip * 2 + (1 - core)
    f32, bf16 = jnp.float32, jnp.bfloat16

    def chunk(c):
        return pl.ds(starts[c], sizes[c])

    ld_w = [pltpu.make_async_copy(src, dst, lsem.at[k]) for k, (src, dst) in
            enumerate(((wq_hbm, wq), (wk_hbm, wk), (wv_hbm, wv), (wo_hbm, wo)))]
    ld_h = [pltpu.make_async_copy(hid_hbm.at[chunk(c)], hid.at[chunk(c)], lsem.at[4 + c]) for c in range(nj)]

    def ld_kv(c):
        sl = pl.ds(starts[c] * per_row, sizes[c] * per_row)
        return [pltpu.make_async_copy(kc_hbm.at[sl], kc.at[sl], csem.at[0, c]),
                pltpu.make_async_copy(vc_hbm.at[sl], vc.at[sl], csem.at[1, c])]

    ld_p = [pltpu.make_async_copy(src, dst, psem.at[k]) for k, (src, dst) in enumerate(
        ((pos_hbm, pos_ref), (tab_hbm, tab_ref), (qw_hbm, qw_ref), (kw_hbm, kw_ref), (pw_hbm, pw_ref)))]
    for cp in [ld_h[0], ld_w[0], ld_w[1]] + ld_p + [ld_w[2], ld_h[1]]:
        cp.start()

    barrier = pltpu.get_barrier_semaphore()
    for d in range(1, n):
        pl.semaphore_signal(barrier, inc=1, device_id={'tp': lax.rem(me + d, n)}, device_id_type=MESH)

    lane = lax.broadcasted_iota(jnp.int32, (LANES, LANES), 1)
    sub = lax.broadcasted_iota(jnp.int32, (LANES, LANES), 0)
    eye = lane == sub
    span = 8 * per_row
    ci = lax.broadcasted_iota(jnp.int32, (16, span), 1)
    ri = lax.broadcasted_iota(jnp.int32, (16, span), 0)
    match = jnp.logical_and(ci // per_row == ri % 8, ci % heads == ri // 8)
    slotm = jnp.where(match, (ci % per_row) // heads, 1000)
    scale2 = (hd ** -0.5) * math.log2(math.e)

    def to_row(col):
        return jnp.sum(jnp.where(eye, jnp.broadcast_to(col, (LANES, LANES)), 0.0), axis=0, keepdims=True)

    def to_col(row):
        return jnp.sum(jnp.where(eye, jnp.broadcast_to(row, (LANES, LANES)), 0.0), axis=1, keepdims=True)

    def energy_copy(c, d):
        return pltpu.make_async_remote_copy(
            src_ref=esend.at[c], dst_ref=erecv.at[c, d - 1], send_sem=essem.at[c, d - 1], recv_sem=ersem.at[c, d - 1],
            device_id={'tp': lax.rem(me + d, n)}, device_id_type=MESH)

    wo_copy = pltpu.make_async_remote_copy(
        src_ref=wo_hbm, dst_ref=wop, send_sem=osem.at[0], recv_sem=osem.at[1],
        device_id={'tp': mate}, device_id_type=MESH)

    def project_qkv(c):
        cs, per = chunk(c), sizes[c] // LANES
        ld_h[c].wait()
        rows_out = []
        for k, (w, f) in enumerate(((wq, qf), (wk, kf))):
            if c == 0:
                ld_w[k].wait()
            val = jnp.dot(hid[cs, :], w[...], preferred_element_type=f32).astype(bf16).astype(f32)
            f[cs, :] = val
            en = jnp.sum(val * val, axis=1, keepdims=True)
            for b in range(per):
                rows_out.append(to_row(en[b * LANES:(b + 1) * LANES]))
            if c == 0 and k == 1:
                for cp in ld_h[2:4] + ld_kv(0) + ld_kv(1) + ld_h[4:] + [ld_w[3]]:
                    cp.start()
        pad = 8 - len(rows_out)
        esend[c] = jnp.concatenate(rows_out + [jnp.zeros((pad, LANES), f32)], axis=0)
        if c == 0:
            pl.semaphore_wait(barrier, n - 1)
        for d in range(1, n):
            energy_copy(c, d).start()
        if c == 0:
            ld_w[2].wait()
            wo_copy.start()
        if 0 < c < nj - 1:
            for cp in ld_kv(c + 1):
                cp.start()
        val = jnp.dot(hid[cs, :], wv[...], preferred_element_type=f32).astype(bf16).astype(f32)
        for h in range(heads):
            vn[h, cs, :] = val[:, h * hd:(h + 1) * hd]

    def norm_rope(c):
        if c == 0:
            for cp in ld_p:
                cp.wait()
        total, per = esend[c], sizes[c] // LANES
        for d in range(1, n):
            energy_copy(c, d).wait_recv()
            total = total + erecv[c, d - 1]
        inv = lax.rsqrt(total / width + NORM_EPS)
        for b in range(per):
            base = starts[c] + b * LANES
            rs = pl.ds(base, LANES)
            p = to_col(pos_ref[starts[c] // LANES + b:starts[c] // LANES + b + 1, :].astype(f32)).astype(jnp.int32)
            pcol[rs, :] = jnp.broadcast_to(p, (LANES, LANES))
            hot = jnp.logical_and(lane < 3 * slots, lane % slots == p)
            trig = jnp.dot(jnp.where(hot, 1.0, 0.0).astype(bf16), tab_ref[...], preferred_element_type=f32)
            cos, sin = trig[:, :hd], trig[:, hd:]
            for f, w_ref, which in ((qf, qw_ref, 0), (kf, kw_ref, 1)):
                scale = to_col(inv[which * per + b:which * per + b + 1, :])
                normed = (f[rs, :] * scale * w_ref[...]).astype(bf16).astype(f32)
                rot = []
                for h in range(heads):
                    x = normed[:, h * hd:(h + 1) * hd]
                    rot.append(x * cos + pltpu.roll(x, hd // 2, 1) * sin)
                if which == 0:
                    grouped = jnp.concatenate([r.reshape(LANES // 8, 8, hd) for r in rot], axis=1)
                    qg[pl.ds(base // 8, LANES // 8)] = grouped.astype(bf16)
                else:
                    for h in range(heads):
                        kn[h, rs, :] = rot[h].astype(bf16).astype(f32)

    def attend_block(i, carry):
        base = i * BLK
        n_grp = BLK // 8

        def kv_rows(g, count):
            return pl.ds(pl.multiple_of(base * per_row + g * span, span), count * span)

        for g in range(n_grp):
            s_scr[pl.ds(g * 16, 16), :] = lax.dot_general(
                qg[i * n_grp + g], kc[kv_rows(g, 1), :], (((1,), (1,)), ((), ())), preferred_element_type=f32)
        p_new = []
        for g in range(n_grp):
            r8 = pl.ds(pl.multiple_of(base + g * 8, 8), 8)
            pc = jnp.concatenate([pcol[r8, :]] * heads, axis=0)
            wide_pc = jnp.concatenate([pc] * (span // LANES), axis=1)
            k_own = jnp.concatenate([kn[h, r8, :] for h in range(heads)], axis=0)
            s_own = jnp.sum(qg[i * n_grp + g].astype(f32) * k_own, axis=1, keepdims=True)
            sc = jnp.where(slotm < wide_pc, s_scr[pl.ds(g * 16, 16), :], NEG)
            top = jnp.maximum(jnp.max(sc, axis=1, keepdims=True), s_own)
            e = jnp.exp2((sc - top) * scale2)
            e_own = jnp.exp2((s_own - top) * scale2)
            inv_l = 1.0 / (jnp.sum(e, axis=1, keepdims=True) + e_own)
            p_scr[pl.ds(g * 16, 16), :] = (e * inv_l).astype(bf16)
            p_new.append((e_own * inv_l).astype(bf16).astype(f32))
        for pair in range(n_grp // 2):
            vv = jnp.concatenate([vc[kv_rows(2 * pair, 1), :], vc[kv_rows(2 * pair + 1, 1), :]], axis=1)
            oo = jnp.dot(p_scr[pl.ds(pair * 32, 32), :], vv, preferred_element_type=f32)
            res = []
            for t in range(2):
                g = 2 * pair + t
                r8 = pl.ds(pl.multiple_of(base + g * 8, 8), 8)
                v_own = jnp.concatenate([vn[h, r8, :] for h in range(heads)], axis=0)
                res.append(oo[16 * t:16 * t + 16, t * hd:(t + 1) * hd] + p_new[g] * v_own)
            rs = pl.ds(pl.multiple_of(base + pair * 16, 16), 16)
            for h in range(heads):
                o_scr[rs, h * hd:(h + 1) * hd] = jnp.concatenate(
                    [res[0][8 * h:8 * h + 8], res[1][8 * h:8 * h + 8]], axis=0).astype(bf16)
        return carry

    def attend(c, piece):
        if piece == 0:
            for cp in ld_kv(c):
                cp.wait()
        first = (starts[c] + piece * LANES) // BLK
        lax.fori_loop(first, first + LANES // BLK, attend_block, 0)

    def mine_of(j):
        return pl.ds(starts[j] // 2, half_of[j])

    def fs(j):
        return pl.ds(starts[j] // (2 * n), hf_of[j])

    def qs(j, y, part_no):
        return pl.ds(pl.multiple_of(starts[j] // 2 + y * own_of[j] + part_no * hf_of[j], hf_of[j]), hf_of[j])

    def os(j, c):
        return pl.ds(pl.multiple_of(starts[j] + c * half_of[j], half_of[j]), half_of[j])

    def gs(j, c, y, part_no=None):
        first = starts[j] + c * half_of[j] + y * own_of[j]
        if part_no is None:
            return pl.ds(pl.multiple_of(first, own_of[j]), own_of[j])
        return pl.ds(pl.multiple_of(first + part_no * hf_of[j], hf_of[j]), hf_of[j])

    def remote(kind, j, src, dst, dev):
        return pltpu.make_async_remote_copy(src_ref=src, dst_ref=dst, send_sem=ssem.at[kind, j], recv_sem=rsem.at[kind, j],
                                            device_id={'tp': dev}, device_id_type=MESH)

    sent = []

    def send(kind, j, src, dst, dev):
        cp = remote(kind, j, src, dst, dev)
        cp.start()
        sent.append(cp)

    def recv(kind, j, dst, dev):
        remote(kind, j, dst, dst, dev).wait_recv()

    def p0(j):
        send(O, j, o_scr.at[os(j, 1 - core)], opart.at[mine_of(j)], mate)

    def p1(j):
        if j == 0:
            ld_w[3].wait()
            wo_copy.wait_recv()
        recv(O, j, opart.at[mine_of(j)], mate)
        mine = o_scr[os(j, core), :]
        theirs = opart[mine_of(j), :]
        step = 512
        for c0 in range(0, width, step):
            acc = jnp.dot(mine, wo[:, c0:c0 + step], preferred_element_type=f32)
            acc = acc + jnp.dot(theirs, wop[:, c0:c0 + step], preferred_element_type=f32)
            part[mine_of(j), c0:c0 + step] = acc.astype(bf16)
        send(A_R, j, part.at[qs(j, xa, 0)], ra.at[0, fs(j)], right)
        send(A_L, j, part.at[qs(j, xa, 1)], ra.at[1, fs(j)], left)
        send(B_R, j, part.at[qs(j, xr, 1)], rb.at[0, fs(j)], right)
        send(B_L, j, part.at[qs(j, xl, 0)], rb.at[1, fs(j)], left)

    def p2(j):
        for k in range(2):
            recv((A_R, A_L)[k], j, ra.at[k, fs(j)], (left, right)[k])
            own_part = part[qs(j, (xr, xl)[k], k), :].astype(f32)
            cst[k, fs(j), :] = (own_part + ra[k, fs(j), :].astype(f32)).astype(bf16)
            send((C_R, C_L)[k], j, cst.at[k, fs(j)], rc.at[k, fs(j)], (right, left)[k])

    def p3(j):
        for k in range(2):
            recv((B_L, B_R)[k], j, rb.at[1 - k, fs(j)], (right, left)[k])
            recv((C_R, C_L)[k], j, rc.at[k, fs(j)], (left, right)[k])
            a = (part[qs(j, chip, k), :].astype(f32) + rc[k, fs(j), :].astype(f32) + rb[1 - k, fs(j), :].astype(f32))
            inv = lax.rsqrt(jnp.sum(a * a, axis=1, keepdims=True) / width + NORM_EPS)
            mine = gs(j, core, chip, k)
            out_ref[mine, :] = (hid[mine, :].astype(f32) + a * inv * pw_ref[...]).astype(bf16)
        blk = out_ref.at[gs(j, core, chip)]
        h0, h1 = out_ref.at[gs(j, core, chip, 0)], out_ref.at[gs(j, core, chip, 1)]
        send(G1_R0, j, h0, h0, right)
        send(G1_L1, j, h1, h1, left)
        send(G1_R1, j, h1, h1, right)
        send(G1_L0, j, h0, h0, left)
        send(D_OWN, j, blk, blk, mate)

    def p4(j):
        bl = [out_ref.at[gs(j, core, xl, k)] for k in range(2)]
        br = [out_ref.at[gs(j, core, xr, k)] for k in range(2)]
        recv(G1_R0, j, bl[0], left)
        send(G2_R, j, bl[0], bl[0], right)
        recv(G1_L1, j, br[1], right)
        send(G2_L, j, br[1], br[1], left)
        recv(G1_R1, j, bl[1], left)
        full_l = out_ref.at[gs(j, core, xl)]
        send(D_LEFT, j, full_l, full_l, mate)
        recv(G1_L0, j, br[0], right)
        full_r = out_ref.at[gs(j, core, xr)]
        send(D_RIGHT, j, full_r, full_r, mate)

    def p5(j):
        b0 = out_ref.at[gs(j, core, xa, 0)]
        recv(G2_R, j, b0, left)
        send(D_ANT0, j, b0, b0, mate)
        b1 = out_ref.at[gs(j, core, xa, 1)]
        recv(G2_L, j, b1, right)
        send(D_ANT1, j, b1, b1, mate)

    new_out = [pltpu.make_async_copy(kn, kn_hbm, nsem.at[0]), pltpu.make_async_copy(vn, vn_hbm, nsem.at[1])]
    stages = dict(Q=project_qkv, R=norm_rope, T=attend, a=p0, b=p1, c=p2, d=p3, e=p4, f=p5)
    for token in ORDER:
        stages[token[0]](*map(int, token[1:].split('.')))
        if token == 'R' + str(nj - 1):
            for cp in new_out:
                cp.start()
    for j in range(nj):
        oc = 1 - core
        recv(D_OWN, j, out_ref.at[gs(j, oc, chip)], mate)
        recv(D_LEFT, j, out_ref.at[gs(j, oc, xl)], mate)
        recv(D_RIGHT, j, out_ref.at[gs(j, oc, xr)], mate)
        recv(D_ANT0, j, out_ref.at[gs(j, oc, xa, 0)], mate)
        recv(D_ANT1, j, out_ref.at[gs(j, oc, xa, 1)], mate)
    for cp in sent:
        cp.wait_send()
    for c in range(nj):
        for d in range(1, n):
            energy_copy(c, d).wait_send()
    wo_copy.wait_send()
    for cp in new_out:
        cp.wait()


def decode_step(n, slots, heads, hd, positions, hidden, w_q, w_k, w_v, w_o, q_norm_w, k_norm_w, post_norm_w, k_flat, v_flat, sizes):
    rows, width = hidden.shape
    cols = heads * hd
    nj = len(sizes)
    span = 8 * slots * heads
    f32, bf16 = jnp.float32, jnp.bfloat16
    dma = pltpu.SemaphoreType.DMA
    return pl.pallas_call(
        functools.partial(step_kernel, n, sizes, slots, heads, hd),
        out_shape=(pltpu.VMEM(k_flat.shape, bf16), pltpu.VMEM(v_flat.shape, bf16), pltpu.VMEM((rows, width), bf16),
                   jax.ShapeDtypeStruct((heads, rows, hd), f32), jax.ShapeDtypeStruct((heads, rows, hd), f32)),
        in_specs=[HBM_SPEC] * 12,
        out_specs=(VMEM_SPEC,) * 3 + (HBM_SPEC,) * 2,
        scratch_shapes=[
            pltpu.VMEM((heads, rows, hd), f32), pltpu.VMEM((heads, rows, hd), f32),
            pltpu.VMEM((rows // LANES, LANES), jnp.int32), pltpu.VMEM((LANES, 2 * hd), bf16), pltpu.VMEM((1, cols), f32),
            pltpu.VMEM((1, cols), f32), pltpu.VMEM((1, width), f32),
            pltpu.VMEM((rows, width), bf16), pltpu.VMEM((width, cols), bf16), pltpu.VMEM((width, cols), bf16),
            pltpu.VMEM((width, cols), bf16), pltpu.VMEM((cols, width), bf16), pltpu.VMEM((cols, width), bf16),
            pltpu.VMEM((rows, cols), f32), pltpu.VMEM((rows, cols), f32), pltpu.VMEM((rows // 8, 8 * heads, hd), bf16),
            pltpu.VMEM((rows, LANES), jnp.int32), pltpu.VMEM((BLK * heads, span), f32), pltpu.VMEM((BLK * heads, span), bf16),
            pltpu.VMEM((rows, cols), bf16), pltpu.VMEM((rows // 2, cols), bf16), pltpu.VMEM((rows // 2, width), bf16),
            pltpu.VMEM((2, rows // (2 * n), width), bf16), pltpu.VMEM((2, rows // (2 * n), width), bf16),
            pltpu.VMEM((2, rows // (2 * n), width), bf16), pltpu.VMEM((2, rows // (2 * n), width), bf16),
            pltpu.VMEM((nj, 8, LANES), f32), pltpu.VMEM((nj, n - 1, 8, LANES), f32),
            dma((4 + nj,)), dma((5,)), dma((2, nj)), dma((2,)), dma((2,)), dma((nj, n - 1)), dma((nj, n - 1)), dma((18, nj)), dma((18, nj)),
        ],
        compiler_params=pltpu.CompilerParams(collective_id=0, has_side_effects=True, vmem_limit_bytes=26 << 20),
        name='decode_step',
    )(positions.reshape(rows // LANES, LANES), jnp.asarray(rope_table(slots, hd)), q_norm_w.reshape(1, cols),
      k_norm_w.reshape(1, cols), post_norm_w.reshape(1, width), hidden, w_q, w_k, w_v, w_o, k_flat, v_flat)


def store_kernel(blk, slots, heads, hd, pos_s, kn, vn, kc, vc, ko, vo, kc_alias, vc_alias, mtab, sem):
    rows = kn.shape[1]
    per_row = slots * heads
    even = lax.broadcasted_iota(jnp.int32, (8, hd), 0) % heads == 0
    pair_id = lax.broadcasted_iota(jnp.int32, (8, hd), 0) // heads
    for k in range(4):
        mtab[k] = jnp.where(pair_id == k, 1.0, 0.0).astype(jnp.bfloat16)

    def copies(i):
        sl = pl.ds(pl.multiple_of(i * blk * per_row, blk * per_row), blk * per_row)
        return [pltpu.make_async_copy(kc_alias.at[sl], ko.at[sl], sem.at[0, i]),
                pltpu.make_async_copy(vc_alias.at[sl], vo.at[sl], sem.at[1, i])]

    def body(i, carry):
        base = i * blk
        for r in range(blk):
            p = pos_s[base + r]
            at = pl.ds(pl.multiple_of((base + r) * per_row + lax.shift_left(lax.shift_right_logical(p, 2), 3), 8), 8)
            hit = mtab[p & 3] > 0
            row = pl.ds(base + r, 8, stride=0)
            for src, dst in ((kn, kc_alias), (vn, vc_alias)):
                new = jnp.where(even, src[0, row, :], src[1, row, :]).astype(jnp.bfloat16)
                dst[at, :] = jnp.where(hit, new, dst[at, :])
        for cp in copies(i):
            cp.start()
        return carry

    lax.fori_loop(0, rows // blk, body, 0)
    for i in range(rows // blk):
        for cp in copies(i):
            cp.wait()


def store(positions, kn, vn, k_vm, v_vm, slots, heads, hd, blk=64):
    rows = kn.shape[1]
    bf16 = jnp.bfloat16
    dma = pltpu.SemaphoreType.DMA
    res = pl.pallas_call(
        functools.partial(store_kernel, blk, slots, heads, hd),
        out_shape=(jax.ShapeDtypeStruct(k_vm.shape, bf16),
                   jax.ShapeDtypeStruct(v_vm.shape, bf16), pltpu.VMEM(k_vm.shape, bf16), pltpu.VMEM(v_vm.shape, bf16)),
        in_specs=[pl.BlockSpec(memory_space=pltpu.SMEM)] + [VMEM_SPEC] * 4,
        out_specs=(HBM_SPEC, HBM_SPEC, VMEM_SPEC, VMEM_SPEC),
        input_output_aliases={3: 2, 4: 3},
        scratch_shapes=[pltpu.VMEM((4, 8, hd), bf16), dma((2, rows // blk))],
        compiler_params=pltpu.CompilerParams(vmem_limit_bytes=26 << 20),
        name='store',
    )(positions, kn, vn, k_vm, v_vm)
    return res[:2]


def chunk_sizes(rows):
    unit = rows // 8
    return [unit * k for k in CHUNKS]


def solution(mesh):
    n = mesh.shape['tp']

    def local_step(hidden, w_q, w_k, w_v, w_o, q_norm_w, k_norm_w, post_norm_w, k_cache, v_cache, positions):
        rows, slots, heads, hd = k_cache.shape
        flat = (rows * slots * heads, hd)
        k_vm, v_vm, hid_vm, kn, vn = decode_step(n, slots, heads, hd, positions, hidden, w_q, w_k, w_v, w_o, q_norm_w,
                                                 k_norm_w, post_norm_w, k_cache.reshape(flat), v_cache.reshape(flat), chunk_sizes(rows))
        k_new, v_new = store(positions, kn, vn, k_vm, v_vm, slots, heads, hd)
        return hid_vm, k_new.reshape(k_cache.shape), v_new.reshape(v_cache.shape)

    cache_spec = P('dp', None, 'tp', None)
    return jax.shard_map(local_step, mesh=mesh, in_specs=(P('dp', None), P(None, 'tp'), P(None, 'tp'), P(None, 'tp'), P('tp', None), P('tp'), P('tp'), P(None), cache_spec, cache_spec, P('dp')), out_specs=(P('dp', None), cache_spec, cache_spec), check_vma=False)
```
